32 devices in a mesh: gx: 8 (over z, core), gy: 4 (over y, x).
Axes of the slice: x: 2, y: 2, z: 4, core: 2. Of those that a mesh axis runs over, the one named last changes fastest.
Arguments:
- mesh_state: bfloat16 [128, 128, 32, 128], P('gx', 'gy'), may hold values from -6 to 6
- part_feat: bfloat16 [131072, 128], P(('gx', 'gy')), may hold values from -6 to 6
- cell_index: int32 [131072], P(('gx', 'gy')), may hold values from 0 to 16383, as said below
- pairs: int32 [2, 786432], P(None, ('gx', 'gy')), may hold values from 0 to 4095, as said below
- dest: int32 [131072], P(('gx', 'gy')), may hold values from 0 to 8, as said below
- mass: float32 [131072], P(('gx', 'gy')), may hold values from 0.5 to 2
- velocity: float32 [3, 131072], P(None, ('gx', 'gy')), may hold values from -30 to 30
- w_enc: bfloat16 [128, 128], replicated, may hold values from -0.5 to 0.5
- w_mesh: bfloat16 [128, 128], replicated, may hold values from -0.21875 to 0.21875
- w_pair: bfloat16 [128, 256], replicated, may hold values from -0.5 to 0.5
- w_edge: bfloat16 [128, 128], replicated, may hold values from -0.5 to 0.5
- w_node: bfloat16 [256, 128], replicated, may hold values from -0.25 to 0.25
- w_accel: bfloat16 [3, 128], replicated, may hold values from -0.5 to 0.5
Outputs:
- mesh_out: bfloat16 [128, 128, 32, 128], P('gx', 'gy')
- stay_feat: bfloat16 [131072, 128], P(('gx', 'gy'))
- stay_vel: float32 [3, 131072], P(None, ('gx', 'gy'))
- arrived_feat: bfloat16 [32768, 128], P(('gx', 'gy'))
- arrived_vel: float32 [4, 32768], P(None, ('gx', 'gy'))
The draws below stay inside these ranges and needn't reach their ends.
Inputs may be any that keep to these rules, and one draw needn't show every extreme that they name: `dest`: 0 means the particle stays; k from 1 to 8 moves it in the k-th direction of the steps. At most 128 particles of one device take any one direction, and some device receives 128 particles from each of its eight neighbours. `cell_index`: A device's particles come in 8 aligned groups of 512 rows; the particles of group g lie in cells g * 2048 to (g + 1) * 2048 - 1 of the device's block. `pairs`: A device's columns come in 8 aligned groups of 3072; both rows of a column of group g name particles of the device's group g, rows g * 512 to (g + 1) * 512 - 1.
All inputs are finite; a program needn't handle non-finite values.
Results may differ from the reference program's by a relative error of at most 0.0085.
Values may be sent and summed in bfloat16 or wider, within the bound.
A program may use at most 128 MiB of HBM per device.

```python
import math
import jax
import jax.numpy as jnp
from jax import lax

F = 128
C = 128
CX = 16
CY = 32
CZ = 32
PART_DEV = 4096
NBR = 6
GRP = 512
NGRP = 8
EDGE_DEV = 24576
CELLS_DEV = 16384
NX = 128
NY = 128
PARTICLES = 131072
EDGES = 786432
N_GX = 8
N_GY = 4
DEVICES = 32


def draw_cell_index(key, part):
    span = CELLS_DEV // NGRP
    row = jnp.arange(PARTICLES, dtype=jnp.int32) % PART_DEV
    group = row // GRP
    local = jax.random.randint(jax.random.fold_in(key, 31), (PARTICLES,), 0, span)
    return (local + group * span).astype(jnp.int32)


def draw_pairs(key, part):
    column = jnp.arange(EDGES, dtype=jnp.int32) % EDGE_DEV
    group = column // (GRP * NBR)
    local = jax.random.randint(jax.random.fold_in(key, 37), (2, EDGES), 0, GRP)
    return (local + group[None, :] * GRP).astype(jnp.int32)


def draw_dest(key, part):
    keys = jax.random.split(jax.random.fold_in(key, 11), 4)
    level = jax.random.randint(keys[0], (DEVICES,), 0, 5)
    rate = 16 * jnp.left_shift(jnp.ones((DEVICES,), jnp.int32), level.astype(jnp.int32))
    target = jax.random.randint(keys[1], (), 0, DEVICES)
    target_x = target // N_GY
    target_y = target % N_GY
    device = jnp.arange(DEVICES, dtype=jnp.int32)
    rel_x = (device // N_GY - target_x + N_GX) % N_GX
    rel_y = (device % N_GY - target_y + N_GY) % N_GY
    near_x = (rel_x <= 1) | (rel_x == N_GX - 1)
    near_y = (rel_y <= 1) | (rel_y == N_GY - 1)
    forced = near_x & near_y
    pick = jax.random.randint(keys[2], (DEVICES, PART_DEV), 0, 1024)
    way = jax.random.randint(keys[3], (DEVICES, PART_DEV), 1, 9)
    cyclic = jnp.arange(PART_DEV, dtype=jnp.int32) % 8 + 1
    chosen = jnp.where(pick < rate[:, None], way, 0)
    chosen = jnp.where(forced[:, None], cyclic[None, :], chosen)
    onehot = (chosen[:, :, None] == jnp.arange(1, 9, dtype=jnp.int32)[None, None, :]).astype(jnp.int32)
    place = jnp.sum(jnp.cumsum(onehot, axis=1) * onehot, axis=2)
    capacity = PART_DEV // 32
    chosen = jnp.where(place > capacity, 0, chosen)
    return chosen.reshape(-1).astype(jnp.int32)


def draw_velocity(key, part):
    keys = jax.random.split(jax.random.fold_in(key, 23), 2)
    device = jnp.arange(PARTICLES, dtype=jnp.int32) // PART_DEV
    ramp = 1.0 + 2.0 * device.astype(jnp.float32) / max(DEVICES - 1, 1)
    common = jax.random.uniform(keys[0], (3, 1), jnp.float32, 0.5, 1.5)
    noise = jnp.clip(jax.random.normal(keys[1], (3, PARTICLES), jnp.float32), -6.0, 6.0)
    return ((noise + common) * ramp[None, :]).astype(jnp.float32)


def steps_of(rng, extent, pieces, smallest, largest):
    loudness, own = 1.0, jax.random.fold_in(rng, 6)
    for axis_at, shards_of in pieces:
        draws = jnp.exp(jax.random.uniform(jax.random.fold_in(own, axis_at), (shards_of,), jnp.float32, smallest / len(pieces), largest / len(pieces)))
        loudness = loudness * jnp.repeat(draws, extent[axis_at] // shards_of).reshape([-1 if axis == axis_at else 1 for axis in range(len(extent))])
    return loudness


def centred(stream_key, dims, scale, reach, shards=(), kind=jnp.bfloat16):
    entries = jax.random.normal(stream_key, dims, jnp.float32) * scale
    if len(shards) > 0:
        entries = steps_of(stream_key, dims, shards, -0.22, 0.18) * entries
    return jnp.clip(entries, min=-reach, max=reach).astype(kind)


def setup_inputs(seed: int = 0) -> dict:
    key_list = jax.random.split(jax.random.key(seed), 14)
    mesh_state = centred(key_list[0], (NX, NY, CZ, C), 1.0, 6.0, ((0, 8), (1, 4)))
    part_feat = centred(key_list[1], (PARTICLES, F), 1.0, 6.0, ((0, 32),))
    cell_index = draw_cell_index(jax.random.fold_in(key_list[13], 71), 0)
    pairs = draw_pairs(jax.random.fold_in(key_list[13], 71), 0)
    dest = draw_dest(jax.random.fold_in(key_list[13], 71), 0)
    mass = jnp.clip(jnp.exp(math.log(2.0) - 1.3862944 * jax.random.uniform(key_list[5], (PARTICLES,), jnp.float32) ** steps_of(key_list[5], (PARTICLES,), ((0, 32),), -0.2, 0.2)), 0.5, 2.0)
    velocity = draw_velocity(jax.random.fold_in(key_list[13], 71), 0)
    w_enc = centred(key_list[7], (F, C), F ** -0.5, 0.5)
    w_mesh = centred(key_list[8], (C, C), (6 * C) ** -0.5, 0.21875)
    w_pair = centred(key_list[9], (F, 2 * F), F ** -0.5, 0.5)
    w_edge = centred(key_list[10], (F, F), F ** -0.5, 0.5)
    w_node = centred(key_list[11], (F + C, F), (4 * F) ** -0.5, 0.25)
    w_accel = centred(key_list[12], (3, F), F ** -0.5, 0.5)
    return {"mesh_state": mesh_state, "part_feat": part_feat, "cell_index": cell_index, "pairs": pairs, "dest": dest, "mass": mass, "velocity": velocity, "w_enc": w_enc, "w_mesh": w_mesh, "w_pair": w_pair, "w_edge": w_edge, "w_node": w_node, "w_accel": w_accel}


directions = ((-1, -1), (-1, 0), (-1, 1), (0, -1), (0, 1), (1, -1), (1, 0), (1, 1))


def encode(state_rows, feat, cell, w_enc):
    deposit = jnp.zeros((state_rows.shape[0], feat.shape[1]), jnp.float32).at[cell].add(feat.astype(jnp.float32))
    deposit = deposit.astype(jnp.bfloat16)
    return (state_rows.astype(jnp.float32) + jnp.dot(deposit, w_enc, preferred_element_type=jnp.float32)).astype(jnp.bfloat16)


def zsides(field):
    padded = jnp.pad(field, [(0, 0)] * (field.ndim - 2) + [(1, 1), (0, 0)])
    return padded[..., 2:, :] + padded[..., :-2, :]


def mesh_update(centre, sides, w_mesh):
    width = centre.shape[-1]
    summed = sides.astype(jnp.bfloat16).reshape(-1, width)
    update = jnp.dot(summed, w_mesh, preferred_element_type=jnp.float32).reshape(centre.shape)
    return (centre.astype(jnp.float32) + jax.nn.silu(update)).astype(jnp.bfloat16)


def particle_step(feat, cell, pair, mesh_rows, w_pair, w_edge, w_node):
    width = feat.shape[1]
    proj = jnp.dot(feat, w_pair, preferred_element_type=jnp.float32).astype(jnp.bfloat16)
    proj_send = proj[:, :width]
    proj_recv = proj[:, width:]
    count = pair.shape[1]
    block = min(12288, count)
    turns = count // block
    senders = pair[0].reshape(turns, block)
    receivers = pair[1].reshape(turns, block)

    def edge_block(total, index):
        pre = proj_send[index[0]].astype(jnp.float32) + proj_recv[index[1]].astype(jnp.float32)
        act = jax.nn.silu(pre).astype(jnp.bfloat16)
        message = jnp.dot(act, w_edge, preferred_element_type=jnp.float32)
        return total.at[index[1]].add(message), None

    start = jnp.zeros((feat.shape[0], width), jnp.float32)
    edge_sum, _ = lax.scan(edge_block, start, (senders, receivers))
    edge_sum = edge_sum.astype(jnp.bfloat16)
    near = mesh_rows[cell]
    update = jnp.dot(edge_sum, w_node[:width], preferred_element_type=jnp.float32)
    update = update + jnp.dot(near, w_node[width:], preferred_element_type=jnp.float32)
    return (feat.astype(jnp.float32) + jax.nn.silu(update)).astype(jnp.bfloat16)


def readout(h_new, w_accel):
    return lax.dot_general(w_accel, h_new, (((1,), (1,)), ((), ())), preferred_element_type=jnp.float32)


def pack(h_new, vel1, mass, dest, cap):
    ways = jnp.arange(1, 9, dtype=jnp.int32)
    onehot = (dest[:, None] == ways[None, :]).astype(jnp.int32)
    slot = jnp.sum((jnp.cumsum(onehot, axis=0) - 1) * onehot, axis=1).astype(jnp.int32)
    group = jnp.where(dest > 0, dest - 1, 8).astype(jnp.int32)
    feats = jnp.zeros((8, cap, h_new.shape[1]), jnp.bfloat16).at[group, slot].set(h_new, mode="drop")
    extra = jnp.concatenate([vel1, mass[None, :]], axis=0).T.astype(jnp.bfloat16)
    moving = jnp.zeros((8, cap, 4), jnp.bfloat16).at[group, slot].set(extra, mode="drop")
    return feats, jnp.transpose(moving, (0, 2, 1))


def unpack(moving, drift):
    values = moving.astype(jnp.float32)
    weight = values[..., 3:4, :]
    speed = jnp.where(weight > 0, values[..., :3, :] - drift[:, None], 0.0)
    return jnp.concatenate([speed, weight], axis=-2)


def to_blocks(whole):
    width = whole.shape[-1]
    grid = whole.reshape(N_GX, CX, N_GY, CY, CZ, width).transpose(0, 2, 1, 3, 4, 5)
    return grid.reshape(N_GX * N_GY, CX * CY * CZ, width)


def from_blocks(blocks):
    width = blocks.shape[-1]
    grid = blocks.reshape(N_GX, N_GY, CX, CY, CZ, width).transpose(0, 2, 1, 3, 4, 5)
    return grid.reshape(CX * N_GX, CY * N_GY, CZ, width)


def stencil(mesh1, w_mesh):
    planes = mesh1.shape[0]

    def one_plane(xpos):
        below = lax.dynamic_index_in_dim(mesh1, (xpos + planes - 1) % planes, 0, keepdims=False).astype(jnp.float32)
        above = lax.dynamic_index_in_dim(mesh1, (xpos + 1) % planes, 0, keepdims=False).astype(jnp.float32)
        centre_raw = lax.dynamic_index_in_dim(mesh1, xpos, 0, keepdims=False)
        centre = centre_raw.astype(jnp.float32)
        sides = below + above + jnp.roll(centre, 1, axis=0) + jnp.roll(centre, -1, axis=0) + zsides(centre)
        return mesh_update(centre_raw, sides, w_mesh)

    return lax.map(one_plane, jnp.arange(planes, dtype=jnp.int32))


def reference(mesh_state, part_feat, cell_index, pairs, dest, mass, velocity, w_enc, w_mesh, w_pair, w_edge, w_node, w_accel):
    devices = N_GX * N_GY
    width = part_feat.shape[1]
    feat_b = part_feat.reshape(devices, PART_DEV, width)
    cell_b = cell_index.reshape(devices, PART_DEV)
    pairs_b = pairs.reshape(2, devices, EDGE_DEV).transpose(1, 0, 2)
    dest_b = dest.reshape(devices, PART_DEV)
    mass_b = mass.reshape(devices, PART_DEV)
    vel_b = velocity.reshape(3, devices, PART_DEV).transpose(1, 0, 2)
    state_b = to_blocks(mesh_state)
    mesh1_b = lax.map(lambda item: encode(item[0], item[1], item[2], w_enc), (state_b, feat_b, cell_b))
    mesh2 = stencil(from_blocks(mesh1_b), w_mesh)
    mesh2_b = to_blocks(mesh2)

    def one_device(item):
        feat, cell, pair, rows, speed = item
        h_new = particle_step(feat, cell, pair, rows, w_pair, w_edge, w_node)
        return h_new, speed + readout(h_new, w_accel)

    h_b, vel1_b = lax.map(one_device, (feat_b, cell_b, pairs_b, mesh2_b, vel_b))
    momentum = jnp.sum(mass_b[:, None, :] * vel1_b, axis=(0, 2))
    drift = momentum / jnp.sum(mass)
    staying = dest_b == 0
    stay_feat = jnp.where(staying[:, :, None], h_b, jnp.zeros_like(h_b)).reshape(-1, width)
    stay_vel = jnp.where(staying[:, None, :], vel1_b - drift[None, :, None], 0.0)
    stay_vel = stay_vel.transpose(1, 0, 2).reshape(3, -1)
    cap = PART_DEV // 32
    feats_b, moving_b = lax.map(lambda item: pack(item[0], item[1], item[2], item[3], cap), (h_b, vel1_b, mass_b, dest_b))
    feats_g = feats_b.reshape(N_GX, N_GY, 8, cap, width)
    moving_g = moving_b.reshape(N_GX, N_GY, 8, 4, cap)
    got_f = []
    got_m = []
    for index, offset in enumerate(directions):
        got_f.append(jnp.roll(feats_g[:, :, index], offset, axis=(0, 1)))
        got_m.append(jnp.roll(moving_g[:, :, index], offset, axis=(0, 1)))
    arrived_feat = jnp.stack(got_f, axis=2).reshape(-1, width)
    arrived = unpack(jnp.stack(got_m, axis=2), drift)
    arrived_vel = arrived.transpose(3, 0, 1, 2, 4).reshape(4, -1)
    return mesh2, stay_feat, stay_vel, arrived_feat, arrived_vel
```

```python
import functools
import jax
import jax.numpy as jnp
from jax import lax
from jax.experimental import pallas as pl
from jax.experimental.pallas import tpu as pltpu
from jax.sharding import PartitionSpec as P

directions = ((-1, -1), (-1, 0), (-1, 1), (0, -1), (0, 1), (1, -1), (1, 0), (1, 1))
LANES = 128
VMEM_LIMIT = 60 * 1024 * 1024
MESH = pl.DeviceIdType.MESH


def group_sizes(parts, cells):
    members = min(512, parts)
    count = parts // members
    return (members, count, cells // count)


def silu(v):
    half = 0.5 * v
    return half + half * jnp.tanh(half)


def f32dot(a, b):
    return jnp.dot(a, b, preferred_element_type=jnp.float32)


def nt_dot(a, b):
    return lax.dot_general(a, b, (((1,), (1,)), ((), ())), preferred_element_type=jnp.float32)


def row_hot(keys, rows, first):
    lanes = lax.broadcasted_iota(jnp.int32, (rows, keys.shape[1]), 0) + first
    return jnp.where(lanes == keys, 1.0, 0.0).astype(jnp.bfloat16)


def down_hot(keys, rows):
    place = lax.broadcasted_iota(jnp.int32, (rows, keys.shape[1]), 0).astype(jnp.float32)
    place = place.astype(jnp.bfloat16)
    keys = keys.astype(jnp.float32).astype(jnp.bfloat16)
    one = jnp.ones((), jnp.bfloat16)
    return jnp.where(place == keys, one, jnp.zeros((), jnp.bfloat16))


def col_hot(cols, start, stop, width):
    lanes = lax.broadcasted_iota(jnp.int32, (LANES, width), 1)
    parts = [
        jnp.where(lanes == cols[:, j : j + 1], 1.0, 0.0).astype(jnp.bfloat16)
        for j in range(start, stop)
    ]
    return jnp.concatenate(parts, axis=0)


def moved_by(axis, distance):
    return lax.rem(lax.axis_index(axis) + distance + lax.axis_size(axis), lax.axis_size(axis))


def greet(places):
    barrier = pltpu.get_barrier_semaphore()
    for dx, dy in places:
        where = (moved_by("gx", dx), moved_by("gy", dy))
        pl.semaphore_signal(barrier, inc=1, device_id=where, device_id_type=MESH)


def front_kernel(
    count,
    plane,
    depth,
    chunk,
    cell_ref,
    cell_tile_ref,
    feat_ref,
    state_ref,
    pairs_ref,
    w_enc_ref,
    w_pair_ref,
    w_edge_ref,
    mesh1_ref,
    edge_ref,
    xlo_ref,
    xhi_ref,
    ylo_ref,
    yhi_ref,
    xsend_ref,
    ysend_ref,
    send_sems,
    recv_sems,
):
    turn = pl.program_id(0)
    span, width = state_ref.shape
    members = feat_ref.shape[0]
    planes = span // plane
    beside = ((1, 0), (-1, 0), (0, 1), (0, -1))

    @pl.when(turn == 0)
    def _():
        greet(beside)

    @pl.when(turn < count)
    def _():
        block = members // 2
        half = span // 2
        base = turn * span
        cols = (cell_tile_ref[0] - base).T
        grown = f32dot(feat_ref[...], w_enc_ref[...])
        low, high = [], []
        for j in range(members // LANES):
            rows = grown[j * LANES : (j + 1) * LANES]
            upper = cols[:, j : j + 1] >= half
            low.append(jnp.where(upper, 0.0, rows))
            high.append(jnp.where(upper, rows, 0.0))
        both = jnp.concatenate(
            [jnp.concatenate(low, axis=0), jnp.concatenate(high, axis=0)], axis=1
        ).astype(jnp.bfloat16)
        cells = cell_ref[...] - base
        keys = jnp.where(cells >= half, cells - half, cells)
        for q in range(half // block):
            gain = f32dot(down_hot(keys - q * block, block), both)
            for part in range(2):
                rows = slice(part * half + q * block, part * half + (q + 1) * block)
                mesh1_ref[rows, :] = (
                    state_ref[rows, :].astype(jnp.float32)
                    + gain[:, part * width : (part + 1) * width]
                ).astype(jnp.bfloat16)
        for p in range(planes):
            first = p * plane
            rows = pl.ds(pl.multiple_of((turn * planes + p) * depth, depth), depth)
            ysend_ref[0, rows, :] = mesh1_ref[first + plane - depth : first + plane, :]
            ysend_ref[1, rows, :] = mesh1_ref[first : first + depth, :]

    @pl.when(turn == 0)
    def _():
        xsend_ref[1] = mesh1_ref[:plane, :]

    @pl.when(turn == count - 1)
    def _():
        xsend_ref[0] = mesh1_ref[span - plane :, :]

    def copies():
        sources = (xsend_ref.at[0], xsend_ref.at[1], ysend_ref.at[0], ysend_ref.at[1])
        targets = (xlo_ref, xhi_ref, ylo_ref, yhi_ref)
        return [
            pltpu.make_async_remote_copy(
                src_ref=sources[k],
                dst_ref=targets[k],
                send_sem=send_sems.at[k],
                recv_sem=recv_sems.at[k],
                device_id=(moved_by("gx", dx), moved_by("gy", dy)),
                device_id_type=MESH,
            )
            for k, (dx, dy) in enumerate(beside)
        ]

    @pl.when(turn == count)
    def _():
        pl.semaphore_wait(pltpu.get_barrier_semaphore(), len(beside))
        for copy in copies():
            copy.start()

    @pl.when(turn >= count)
    def _():
        base = (turn - count) * members
        half = members // 2
        table = nt_dot(w_pair_ref[...].T, feat_ref[...]).astype(jnp.bfloat16)
        tables = [
            jnp.concatenate([table[:width, :half], table[:width, half:]], axis=0),
            jnp.concatenate([table[width:, :half], table[width:, half:]], axis=0),
        ]
        zero = jnp.zeros((), jnp.bfloat16)
        total = jnp.zeros((half, 2 * width), jnp.float32)
        for first in range(0, pairs_ref.shape[1], chunk):
            pre = None
            for end in range(2):
                rows = pairs_ref[end : end + 1, first : first + chunk] - base
                upper = rows >= half
                hot = down_hot(jnp.where(upper, rows - half, rows), half)
                got = f32dot(tables[end], hot)
                picked = jnp.where(upper, got[width:], got[:width])
                pre = picked if pre is None else pre + picked
            act = silu(pre)
            acts = jnp.concatenate(
                [jnp.where(upper, 0.0, act), jnp.where(upper, act, 0.0)], axis=0
            ).astype(jnp.bfloat16)
            total = total + nt_dot(hot, acts)
        total = jnp.concatenate([total[:, :width], total[:, width:]], axis=0)
        edge_ref[...] = f32dot(total.astype(jnp.bfloat16), w_edge_ref[...]).astype(jnp.bfloat16)

    @pl.when(turn == 2 * count - 1)
    def _():
        for copy in copies():
            copy.wait()


def node_kernel(
    plane,
    depth,
    cap,
    below_ref,
    centre_ref,
    above_ref,
    xlo_ref,
    xhi_ref,
    ylo_ref,
    yhi_ref,
    cell_ref,
    dest_ref,
    dest_row_ref,
    edge_ref,
    feat_ref,
    mass_ref,
    vel_ref,
    w_mesh_ref,
    w_node_ref,
    w_accel_ref,
    mesh_ref,
    stay_ref,
    vel1_ref,
    packed_ref,
    total_ref,
    slots_ref,
    carry_ref,
):
    step = pl.program_id(0)
    last = pl.num_programs(0) - 1
    span, width = centre_ref.shape
    members = feat_ref.shape[0]
    planes = span // plane
    base = step * span

    @pl.when(step == 0)
    def _():
        slots_ref[...] = jnp.zeros_like(slots_ref)
        carry_ref[...] = jnp.zeros_like(carry_ref)
        total_ref[...] = jnp.zeros_like(total_ref)

    level = lax.broadcasted_iota(jnp.int32, (plane, width), 0) % depth
    for p in range(planes):
        rows = slice(p * plane, (p + 1) * plane)
        centre = centre_ref[rows, :].astype(jnp.float32)
        if p == 0:
            below = jnp.where(
                step == 0, xlo_ref[...].astype(jnp.float32), below_ref[...].astype(jnp.float32)
            )
        else:
            below = centre_ref[(p - 1) * plane : p * plane, :].astype(jnp.float32)
        if p == planes - 1:
            above = jnp.where(
                step == last, xhi_ref[...].astype(jnp.float32), above_ref[...].astype(jnp.float32)
            )
        else:
            above = centre_ref[(p + 1) * plane : (p + 2) * plane, :].astype(jnp.float32)
        edge = slice(p * depth, (p + 1) * depth)
        left = jnp.concatenate([ylo_ref[edge, :].astype(jnp.float32), centre[:-depth]], axis=0)
        right = jnp.concatenate([centre[depth:], yhi_ref[edge, :].astype(jnp.float32)], axis=0)
        down = jnp.where(level == 0, 0.0, pltpu.roll(centre, 1, 0))
        up = jnp.where(level == depth - 1, 0.0, pltpu.roll(centre, plane - 1, 0))
        sides = (below + above + left + right + (up + down)).astype(jnp.bfloat16)
        mesh_ref[rows, :] = (centre + silu(f32dot(sides, w_mesh_ref[...]))).astype(jnp.bfloat16)

    cell_cols = (cell_ref[0] - base).T
    dest_cols = dest_ref[0].T
    turns = members // LANES
    near = f32dot(col_hot(cell_cols, 0, turns, span), mesh_ref[...]).astype(jnp.bfloat16)
    update = f32dot(edge_ref[...], w_node_ref[:width, :]) + f32dot(near, w_node_ref[width:, :])
    h_new = (feat_ref[...].astype(jnp.float32) + silu(update)).astype(jnp.bfloat16)
    h_wide = h_new.astype(jnp.float32)
    for j in range(turns):
        rows = slice(j * LANES, (j + 1) * LANES)
        stay_ref[rows, :] = jnp.where(dest_cols[:, j : j + 1] == 0, h_wide[rows], 0.0).astype(
            jnp.bfloat16
        )
    accel = lax.dot_general(
        w_accel_ref[...], h_new, (((1,), (1,)), ((), ())), preferred_element_type=jnp.float32
    )
    vel1 = vel_ref[...] + accel[:3]
    mass = mass_ref[0]
    vel1_ref[...] = vel1
    sums = jnp.concatenate([mass * vel1, mass], axis=0)
    total_ref[...] += sum(sums[:, j * LANES : (j + 1) * LANES] for j in range(turns))

    dest = dest_row_ref[0]
    ways = lax.broadcasted_iota(jnp.int32, (8, members), 0) + 1
    chosen_way = jnp.where(ways == dest, 1.0, 0.0)
    earlier = jnp.where(
        lax.broadcasted_iota(jnp.int32, (members, members), 0)
        < lax.broadcasted_iota(jnp.int32, (members, members), 1),
        1.0,
        0.0,
    ).astype(jnp.bfloat16)
    place = f32dot(chosen_way.astype(jnp.bfloat16), earlier) + carry_ref[:, :1]
    slot = jnp.sum(place * chosen_way, axis=0, keepdims=True).astype(jnp.int32)
    carry_ref[...] += jnp.sum(chosen_way, axis=1, keepdims=True)
    key = jnp.where(dest > 0, (dest - 1) * cap + slot, -1)
    extra = jnp.concatenate([vel1, mass, jnp.zeros((LANES - 4, members), jnp.float32)], axis=0)
    values = jnp.concatenate([h_new, extra.T.astype(jnp.bfloat16)], axis=1)
    half = slots_ref.shape[0] // 2
    for first in (0, half):
        rows = slice(first, first + half)
        slots_ref[rows, :] += f32dot(row_hot(key, half, first), values)

    @pl.when(step == last)
    def _():
        moving = slots_ref[:, width:].T
        for k in range(8):
            rows = slice(k * cap, (k + 1) * cap)
            packed_ref[k, :cap, :] = slots_ref[rows, :width].astype(jnp.bfloat16)
            packed_ref[k, cap:, :] = moving[:16, rows].astype(jnp.bfloat16)


def meeting_places(nx, ny):
    around = [(o, 0) for o in range(1, nx)] + [(0, o) for o in range(1, ny)]
    around += [(dx % nx, dy % ny) for dx, dy in directions]
    return [place for place in dict.fromkeys(around) if place != (0, 0)]


def tail_kernel(
    nx,
    ny,
    cap,
    packed_ref,
    totals_ref,
    vel1_ref,
    dest_ref,
    feat_ref,
    arrived_ref,
    stay_ref,
    xsum_ref,
    part_ref,
    ysum_ref,
    got_ref,
    send_x,
    recv_x,
    send_y,
    recv_y,
    send_f,
    recv_f,
    send_m,
    recv_m,
):
    me_x, me_y = lax.axis_index("gx"), lax.axis_index("gy")
    places = meeting_places(nx, ny)
    greet(places)
    xsum_ref[me_x] = totals_ref[...]
    pl.semaphore_wait(pltpu.get_barrier_semaphore(), len(places))

    def copy(source, target, sends, recvs, n, dx, dy):
        made = pltpu.make_async_remote_copy(
            src_ref=source,
            dst_ref=target,
            send_sem=sends.at[n],
            recv_sem=recvs.at[n],
            device_id=(moved_by("gx", dx), moved_by("gy", dy)),
            device_id_type=MESH,
        )
        made.start()
        return made

    along_x = [
        copy(totals_ref, xsum_ref.at[me_x], send_x, recv_x, o - 1, o, 0) for o in range(1, nx)
    ]
    moving = [
        copy(packed_ref.at[k, pl.ds(cap, 16)], got_ref.at[k], send_m, recv_m, k, dx, dy)
        for k, (dx, dy) in enumerate(directions)
    ]
    feats = [
        copy(
            packed_ref.at[k, pl.ds(0, cap)],
            feat_ref.at[pl.ds(k * cap, cap)],
            send_f,
            recv_f,
            k,
            dx,
            dy,
        )
        for k, (dx, dy) in enumerate(directions)
    ]
    for made in along_x:
        made.wait()
    part = jnp.sum(xsum_ref[...], axis=0)
    part_ref[...] = part
    ysum_ref[me_y] = part
    along_y = [
        copy(part_ref, ysum_ref.at[me_y], send_y, recv_y, o - 1, 0, o) for o in range(1, ny)
    ]
    for made in along_y:
        made.wait()
    sums = jnp.sum(jnp.sum(ysum_ref[...], axis=0), axis=1, keepdims=True)
    drift = sums[:3] / sums[3:4]
    stay_ref[...] = jnp.where(dest_ref[...] == 0, vel1_ref[...] - drift, 0.0)
    for made in moving:
        made.wait()
    for k in range(len(directions)):
        values = got_ref[k].astype(jnp.float32)
        weight = values[3:4]
        slots = slice(k * cap, (k + 1) * cap)
        arrived_ref[:3, slots] = jnp.where(weight > 0, values[:3] - drift, 0.0)
        arrived_ref[3:4, slots] = weight
    for made in feats:
        made.wait()


def whole(shape):
    return pl.BlockSpec(shape, lambda g: (0,) * len(shape))


def shards(
    mesh_state,
    part_feat,
    cell_index,
    pairs,
    dest,
    mass,
    velocity,
    w_enc,
    w_mesh,
    w_pair,
    w_edge,
    w_node,
    w_accel,
):
    shape = mesh_state.shape
    parts, width = part_feat.shape
    cx, cy, cz, channels = shape
    cells = cx * cy * cz
    plane = cy * cz
    members, count, span = group_sizes(parts, cells)
    planes = span // plane
    per_group = pairs.shape[1] // count
    cap = parts // 32
    nx, ny = lax.axis_size("gx"), lax.axis_size("gy")
    bf16, f32 = (jnp.bfloat16, jnp.float32)
    params = pltpu.CompilerParams(vmem_limit_bytes=VMEM_LIMIT)

    by_rows = pl.BlockSpec((members, width), lambda g: (g, 0))
    by_cells = pl.BlockSpec((span, channels), lambda g: (g, 0))
    by_row = pl.BlockSpec((1, 1, members), lambda g: (g, 0, 0))
    by_tile = pl.BlockSpec((1, members // LANES, LANES), lambda g: (g, 0, 0))

    cell_tile = cell_index.reshape(count, members // LANES, LANES)
    dest_row = dest.reshape(count, 1, members)
    dest_tile = dest.reshape(count, members // LANES, LANES)
    mass_row = mass.reshape(count, 1, members)
    accel8 = jnp.pad(w_accel, ((0, 8 - w_accel.shape[0]), (0, 0)))

    early = lambda g: jnp.minimum(g, count - 1)
    late = lambda g: jnp.maximum(g - count, 0)
    anywhere = pl.BlockSpec(memory_space=pl.ANY)
    mesh1, edge_sum, xlo, xhi, ylo, yhi = pl.pallas_call(
        functools.partial(front_kernel, count, plane, cz, 512 if per_group % 512 == 0 else LANES),
        grid=(2 * count,),
        out_shape=(
            jax.ShapeDtypeStruct((cells, channels), bf16),
            jax.ShapeDtypeStruct((parts, width), bf16),
            jax.ShapeDtypeStruct((plane, channels), bf16),
            jax.ShapeDtypeStruct((plane, channels), bf16),
            jax.ShapeDtypeStruct((cx * cz, channels), bf16),
            jax.ShapeDtypeStruct((cx * cz, channels), bf16),
        ),
        in_specs=[
            pl.BlockSpec((1, members), lambda g: (0, early(g))),
            pl.BlockSpec((1, members // LANES, LANES), lambda g: (early(g), 0, 0)),
            pl.BlockSpec((members, width), lambda g: (lax.rem(g, count), 0)),
            pl.BlockSpec((span, channels), lambda g: (early(g), 0)),
            pl.BlockSpec((2, per_group), lambda g: (0, late(g))),
            whole(w_enc.shape),
            whole(w_pair.shape),
            whole(w_edge.shape),
        ],
        out_specs=(
            pl.BlockSpec((span, channels), lambda g: (early(g), 0)),
            pl.BlockSpec((members, width), lambda g: (late(g), 0)),
            anywhere,
            anywhere,
            anywhere,
            anywhere,
        ),
        scratch_shapes=[
            pltpu.VMEM((2, plane, channels), bf16),
            pltpu.VMEM((2, cx * cz, channels), bf16),
            pltpu.SemaphoreType.DMA((4,)),
            pltpu.SemaphoreType.DMA((4,)),
        ],
        compiler_params=pltpu.CompilerParams(
            vmem_limit_bytes=VMEM_LIMIT, collective_id=0, has_side_effects=True
        ),
        name="front",
    )(
        cell_index.reshape(1, parts),
        cell_tile,
        part_feat,
        mesh_state.reshape(cells, channels),
        pairs,
        w_enc,
        w_pair,
        w_edge,
    )

    one_plane = lambda f: pl.BlockSpec((plane, channels), f)
    by_layer = pl.BlockSpec((planes * cz, channels), lambda g: (g, 0))
    by_speed = pl.BlockSpec((3, members), lambda g: (0, g))
    mesh2, stay_feat, vel1, packed, totals = pl.pallas_call(
        functools.partial(node_kernel, plane, cz, cap),
        grid=(count,),
        out_shape=(
            jax.ShapeDtypeStruct((cells, channels), bf16),
            jax.ShapeDtypeStruct((parts, width), bf16),
            jax.ShapeDtypeStruct((3, parts), f32),
            jax.ShapeDtypeStruct((8, cap + 16, width), bf16),
            jax.ShapeDtypeStruct((4, LANES), f32),
        ),
        in_specs=[
            one_plane(lambda g: (jnp.maximum(g * planes - 1, 0), 0)),
            by_cells,
            one_plane(lambda g: (jnp.minimum(g * planes + planes, cx - 1), 0)),
            whole((plane, channels)),
            whole((plane, channels)),
            by_layer,
            by_layer,
            by_tile,
            by_tile,
            by_row,
            by_rows,
            by_rows,
            by_row,
            by_speed,
            whole(w_mesh.shape),
            whole(w_node.shape),
            whole(accel8.shape),
        ],
        out_specs=(
            by_cells,
            by_rows,
            by_speed,
            whole((8, cap + 16, width)),
            whole((4, LANES)),
        ),
        scratch_shapes=[
            pltpu.VMEM((8 * cap, width + LANES), f32),
            pltpu.VMEM((8, LANES), f32),
        ],
        compiler_params=params,
        name="nodes",
    )(
        mesh1,
        mesh1,
        mesh1,
        xlo,
        xhi,
        ylo,
        yhi,
        cell_tile,
        dest_tile,
        dest_row,
        edge_sum,
        part_feat,
        mass_row,
        velocity,
        w_mesh,
        w_node,
        accel8,
    )

    inside = pl.BlockSpec(memory_space=pltpu.VMEM)
    dma = lambda n: pltpu.SemaphoreType.DMA((n,))
    arrived_feat, arrived_vel, stay_vel = pl.pallas_call(
        functools.partial(tail_kernel, nx, ny, cap),
        out_shape=(
            jax.ShapeDtypeStruct((8 * cap, width), bf16),
            jax.ShapeDtypeStruct((4, 8 * cap), f32),
            jax.ShapeDtypeStruct((3, parts), f32),
        ),
        in_specs=[inside] * 4,
        out_specs=(anywhere, inside, inside),
        scratch_shapes=[
            pltpu.VMEM((nx, 4, LANES), f32),
            pltpu.VMEM((4, LANES), f32),
            pltpu.VMEM((ny, 4, LANES), f32),
            pltpu.VMEM((8, 16, LANES), bf16),
            dma(nx - 1),
            dma(nx - 1),
            dma(ny - 1),
            dma(ny - 1),
            dma(8),
            dma(8),
            dma(8),
            dma(8),
        ],
        compiler_params=pltpu.CompilerParams(
            vmem_limit_bytes=16 * 1024 * 1024, collective_id=1, has_side_effects=True
        ),
        name="tail",
    )(packed, totals, vel1, dest.reshape(1, parts))
    return (mesh2.reshape(shape), stay_feat, stay_vel, arrived_feat, arrived_vel)


def solution(mesh):
    placed = (
        P("gx", "gy", None, None),
        P(("gx", "gy"), None),
        P(("gx", "gy")),
        P(None, ("gx", "gy")),
        P(("gx", "gy")),
        P(("gx", "gy")),
        P(None, ("gx", "gy")),
        P(),
        P(),
        P(),
        P(),
        P(),
        P(),
    )
    return jax.shard_map(
        shards,
        mesh=mesh,
        in_specs=placed,
        out_specs=(
            P("gx", "gy", None, None),
            P(("gx", "gy"), None),
            P(None, ("gx", "gy")),
            P(("gx", "gy"), None),
            P(None, ("gx", "gy")),
        ),
        check_vma=False,
    )
```

```python
import functools
import jax
import jax.numpy as jnp
from jax import lax
from jax.experimental import pallas as pl
from jax.experimental.pallas import tpu as pltpu
from jax.sharding import PartitionSpec as P

directions = ((-1, -1), (-1, 0), (-1, 1), (0, -1), (0, 1), (1, -1), (1, 0), (1, 1))
LANES = 128
VMEM_LIMIT = 60 * 1024 * 1024
CHUNK = 512
MESH = pl.DeviceIdType.MESH


def group_sizes(parts, cells):
    members = min(512, parts)
    count = parts // members
    return (members, count, cells // count)


def silu_of_twice(half):
    return half + half * jnp.tanh(half)


def f32dot(a, b):
    return jnp.dot(a, b, preferred_element_type=jnp.float32)


def nt_dot(a, b):
    return lax.dot_general(a, b, (((1,), (1,)), ((), ())), preferred_element_type=jnp.float32)


def down_hot(keys, rows):
    place = lax.broadcasted_iota(jnp.int32, (rows, keys.shape[1]), 0).astype(jnp.float32)
    place = place.astype(jnp.bfloat16)
    keys = keys.astype(jnp.float32).astype(jnp.bfloat16)
    one = jnp.ones((), jnp.bfloat16)
    return jnp.where(place == keys, one, jnp.zeros((), jnp.bfloat16))


def over_hot(keys, width):
    place = lax.broadcasted_iota(jnp.int32, (keys.shape[0], width), 1).astype(jnp.int16)
    keys = jnp.broadcast_to(keys, (keys.shape[0], LANES)).astype(jnp.int16)
    keys = jnp.concatenate([keys] * (width // LANES), axis=1)
    return jnp.where(place == keys, jnp.ones((), jnp.bfloat16), jnp.zeros((), jnp.bfloat16))


def moved_by(axis, distance):
    return lax.rem(lax.axis_index(axis) + distance + lax.axis_size(axis), lax.axis_size(axis))


def greet(places):
    barrier = pltpu.get_barrier_semaphore()
    for dx, dy in places:
        where = (moved_by("gx", dx), moved_by("gy", dy))
        pl.semaphore_signal(barrier, inc=1, device_id=where, device_id_type=MESH)


def front_kernel(
    turns,
    plane,
    depth,
    chunk,
    cell_ref,
    cell_tile_ref,
    enc_feat_ref,
    state_ref,
    feat_ref,
    pairs_ref,
    w_enc_ref,
    w_pair_ref,
    w_edge_ref,
    mesh1_ref,
    edge_ref,
    xlo_ref,
    xhi_ref,
    ylo_ref,
    yhi_ref,
    xsend_ref,
    ysend_ref,
    half_pair_ref,
    send_sems,
    recv_sems,
):
    turn = pl.program_id(0)
    last = pl.num_programs(0) - 1
    members, width = feat_ref.shape
    groups = cell_tile_ref.shape[0]
    span = state_ref.shape[0] // groups
    planes = state_ref.shape[0] // plane
    beside = ((1, 0), (-1, 0), (0, 1), (0, -1))
    half = members // 2

    def copies():
        sources = (xsend_ref.at[0], xsend_ref.at[1], ysend_ref.at[0], ysend_ref.at[1])
        targets = (xlo_ref, xhi_ref, ylo_ref, yhi_ref)
        return [
            pltpu.make_async_remote_copy(
                src_ref=sources[k],
                dst_ref=targets[k],
                send_sem=send_sems.at[k],
                recv_sem=recv_sems.at[k],
                device_id=(moved_by("gx", dx), moved_by("gy", dy)),
                device_id_type=MESH,
            )
            for k, (dx, dy) in enumerate(beside)
        ]

    @pl.when(turn == 0)
    def _():
        greet(beside)
        half_pair_ref[...] = (0.5 * w_pair_ref[...].astype(jnp.float32)).T.astype(jnp.bfloat16)

    @pl.when(turn == turns)
    def _():
        pl.semaphore_wait(pltpu.get_barrier_semaphore(), len(beside))
        for copy in copies():
            copy.start()

    @pl.when(turn < turns)
    def _():
        top = span // 2
        for g in range(groups):
            base = (turn * groups + g) * span
            mine = slice(g * members, (g + 1) * members)
            cols = (cell_tile_ref[g] - base).T
            grown = f32dot(enc_feat_ref[mine, :], w_enc_ref[...])
            low, high = [], []
            for j in range(members // LANES):
                rows = grown[j * LANES : (j + 1) * LANES]
                upper = cols[:, j : j + 1] >= top
                low.append(jnp.where(upper, 0.0, rows))
                high.append(jnp.where(upper, rows, 0.0))
            both = jnp.concatenate(
                [jnp.concatenate(low, axis=0), jnp.concatenate(high, axis=0)], axis=1
            ).astype(jnp.bfloat16)
            cells = cell_ref[:, mine] - base
            keys = jnp.where(cells >= top, cells - top, cells)
            for q in range(top // half):
                gain = f32dot(down_hot(keys - q * half, half), both)
                for part in range(2):
                    first = g * span + part * top + q * half
                    rows = slice(first, first + half)
                    mesh1_ref[rows, :] = (
                        state_ref[rows, :].astype(jnp.float32)
                        + gain[:, part * width : (part + 1) * width]
                    ).astype(jnp.bfloat16)
        for p in range(planes):
            first = p * plane
            rows = pl.ds(pl.multiple_of((turn * planes + p) * depth, depth), depth)
            ysend_ref[0, rows, :] = mesh1_ref[first + plane - depth : first + plane, :]
            ysend_ref[1, rows, :] = mesh1_ref[first : first + depth, :]

    @pl.when(turn == 0)
    def _():
        xsend_ref[1] = mesh1_ref[:plane, :]

    @pl.when(turn == turns - 1)
    def _():
        xsend_ref[0] = mesh1_ref[(planes - 1) * plane :, :]

    base = turn * members
    table = nt_dot(half_pair_ref[...], feat_ref[...]).astype(jnp.bfloat16)
    tables = [
        jnp.concatenate([table[:width, :half], table[:width, half:]], axis=0),
        jnp.concatenate([table[width:, :half], table[width:, half:]], axis=0),
    ]
    total = jnp.zeros((half, 2 * width), jnp.float32)
    for first in range(0, pairs_ref.shape[1], chunk):
        pre = None
        for end in range(2):
            rows = pairs_ref[end : end + 1, first : first + chunk] - base
            upper = rows >= half
            hot = down_hot(jnp.where(upper, rows - half, rows), half)
            got = f32dot(tables[end], hot)
            picked = jnp.where(upper, got[width:], got[:width])
            pre = picked if pre is None else pre + picked
        act = silu_of_twice(pre).astype(jnp.bfloat16)
        share = jnp.where(upper, 1.0, 0.0)
        acts = jnp.concatenate(
            [act * (1.0 - share).astype(jnp.bfloat16), act * share.astype(jnp.bfloat16)], axis=0
        )
        total = total + nt_dot(hot, acts)
    total = jnp.concatenate([total[:, :width], total[:, width:]], axis=0)
    edge_ref[...] = f32dot(total.astype(jnp.bfloat16), w_edge_ref[...]).astype(jnp.bfloat16)

    @pl.when(turn == last)
    def _():
        for copy in copies():
            copy.wait()


def node_kernel(
    plane,
    depth,
    cap,
    below_ref,
    centre_ref,
    above_ref,
    xlo_ref,
    xhi_ref,
    ylo_ref,
    yhi_ref,
    cell_ref,
    dest_ref,
    dest_row_ref,
    edge_ref,
    feat_ref,
    mass_ref,
    vel_ref,
    w_mesh_ref,
    w_node_ref,
    w_accel_ref,
    mesh_ref,
    stay_ref,
    vel1_ref,
    packed_ref,
    total_ref,
    slots_ref,
    carry_ref,
    near_w_ref,
    wide_w_ref,
    node_w_ref,
    before_ref,
):
    step = pl.program_id(0)
    last = pl.num_programs(0) - 1
    span, width = centre_ref.shape
    members = feat_ref.shape[0]
    planes = span // plane
    base = step * span
    block = 2 * LANES

    @pl.when(step == 0)
    def _():
        slots_ref[...] = jnp.zeros_like(slots_ref)
        carry_ref[...] = jnp.zeros_like(carry_ref)
        total_ref[...] = jnp.zeros_like(total_ref)
        row = lax.broadcasted_iota(jnp.int32, (block, block), 0)
        col = lax.broadcasted_iota(jnp.int32, (block, block), 1)
        gap = row - col
        up_down = (jnp.abs(gap) == 1) & (row // depth == col // depth)
        near_w_ref[...] = jnp.where(up_down | (jnp.abs(gap) == depth), 1.0, 0.0).astype(
            jnp.bfloat16
        )
        scaled = 0.5 * w_mesh_ref[...].astype(jnp.float32)
        none = jnp.zeros_like(scaled)
        wide_w_ref[...] = jnp.concatenate(
            [
                jnp.concatenate([scaled, none], axis=1),
                jnp.concatenate([none, scaled], axis=1),
            ],
            axis=0,
        ).astype(jnp.bfloat16)
        node_w_ref[...] = (0.5 * w_node_ref[...].astype(jnp.float32)).astype(jnp.bfloat16)
        before_ref[...] = jnp.where(
            lax.broadcasted_iota(jnp.int32, (LANES, LANES), 0)
            < lax.broadcasted_iota(jnp.int32, (LANES, LANES), 1),
            1.0,
            0.0,
        ).astype(jnp.bfloat16)

    def wide(rows):
        return rows.astype(jnp.float32)

    for p in range(planes):
        for pair in range(0, plane, 2 * block):
            firsts = [p * plane + pair, p * plane + pair + block]
            raw = [centre_ref[f : f + block, :] for f in firsts]
            around = f32dot(near_w_ref[...], jnp.concatenate(raw, axis=1))
            sides = []
            for n, f in enumerate(firsts):
                rows = slice(f, f + block)
                inner = slice(f - p * plane, f - p * plane + block)
                if p == 0:
                    below = jnp.where(step == 0, xlo_ref[inner, :], below_ref[inner, :])
                else:
                    below = centre_ref[f - plane : f - plane + block, :]
                if p == planes - 1:
                    above = jnp.where(step == last, xhi_ref[inner, :], above_ref[inner, :])
                else:
                    above = centre_ref[f + plane : f + plane + block, :]
                if inner.start == 0:
                    left = ylo_ref[p * depth : (p + 1) * depth, :]
                else:
                    left = centre_ref[f - depth : f, :]
                if inner.stop == plane:
                    right = yhi_ref[p * depth : (p + 1) * depth, :]
                else:
                    right = centre_ref[f + block : f + block + depth, :]
                total = around[:, n * width : (n + 1) * width] + (wide(below) + wide(above))
                sides.append(
                    jnp.concatenate(
                        [
                            total[:depth] + wide(left),
                            total[depth:-depth],
                            total[-depth:] + wide(right),
                        ],
                        axis=0,
                    ).astype(jnp.bfloat16)
                )
            gain = silu_of_twice(f32dot(jnp.concatenate(sides, axis=1), wide_w_ref[...]))
            for n, f in enumerate(firsts):
                mesh_ref[f : f + block, :] = (
                    wide(raw[n]) + gain[:, n * width : (n + 1) * width]
                ).astype(jnp.bfloat16)

    turns = members // LANES
    top = span // 2
    cell_cols = (cell_ref[0] - base).T
    dest_cols = dest_ref[0].T
    hots, uppers = [], []
    for j in range(turns):
        col = cell_cols[:, j : j + 1]
        upper = col >= top
        uppers.append(upper)
        hots.append(over_hot(jnp.where(upper, col - top, col), top))
    pair = jnp.concatenate([mesh_ref[:top, :], mesh_ref[top:, :]], axis=1)
    found = f32dot(jnp.concatenate(hots, axis=0), pair)
    near = jnp.concatenate(
        [
            jnp.where(
                uppers[j],
                found[j * LANES : (j + 1) * LANES, width:],
                found[j * LANES : (j + 1) * LANES, :width],
            )
            for j in range(turns)
        ],
        axis=0,
    ).astype(jnp.bfloat16)
    update = f32dot(jnp.concatenate([edge_ref[...], near], axis=1), node_w_ref[...])
    h_new = (wide(feat_ref[...]) + silu_of_twice(update)).astype(jnp.bfloat16)
    h_wide = h_new.astype(jnp.float32)
    for j in range(turns):
        rows = slice(j * LANES, (j + 1) * LANES)
        stay_ref[rows, :] = jnp.where(dest_cols[:, j : j + 1] == 0, h_wide[rows], 0.0).astype(
            jnp.bfloat16
        )
    vel1 = vel_ref[...] + nt_dot(w_accel_ref[...], h_new)
    mass = mass_ref[...]
    vel1_ref[...] = vel1
    sums = jnp.concatenate([mass * vel1, mass], axis=0)
    total_ref[...] += sum(sums[:, j * LANES : (j + 1) * LANES] for j in range(turns))

    dest = dest_row_ref[...]
    ways = lax.broadcasted_iota(jnp.int32, (8, members), 0) + 1
    chosen = jnp.where(ways == dest, 1.0, 0.0)
    stacked = jnp.concatenate([chosen[:, j * LANES : (j + 1) * LANES] for j in range(turns)], axis=0)
    earlier = f32dot(stacked.astype(jnp.bfloat16), before_ref[...])
    counts = jnp.sum(stacked, axis=1, keepdims=True)
    done = carry_ref[:, :1]
    places = []
    for j in range(turns):
        rows = slice(8 * j, 8 * (j + 1))
        places.append(jnp.where(stacked[rows] > 0, earlier[rows] + done, -1.0))
        done = done + counts[rows]
    carry_ref[...] = jnp.broadcast_to(done, carry_ref.shape)
    place = jnp.concatenate(places, axis=1)
    extra = jnp.concatenate([vel1, mass, jnp.zeros((LANES - 4, members), jnp.float32)], axis=0)
    values = jnp.concatenate([h_new, extra.T.astype(jnp.bfloat16)], axis=1)
    for k in range(8):
        rows = slice(k * cap, (k + 1) * cap)
        slots_ref[rows, :] += f32dot(down_hot(place[k : k + 1], cap), values).astype(jnp.bfloat16)

    @pl.when(step == last)
    def _():
        moving = wide(slots_ref[:, width:]).T
        for k in range(8):
            rows = slice(k * cap, (k + 1) * cap)
            packed_ref[k, :cap, :] = slots_ref[rows, :width]
            packed_ref[k, cap:, :] = moving[:16, rows].astype(jnp.bfloat16)


def meeting_places(nx, ny):
    around = [(o, 0) for o in range(1, nx)] + [(0, o) for o in range(1, ny)]
    around += [(dx % nx, dy % ny) for dx, dy in directions]
    return [place for place in dict.fromkeys(around) if place != (0, 0)]


def tail_kernel(
    nx,
    ny,
    cap,
    packed_ref,
    totals_ref,
    vel1_ref,
    dest_ref,
    feat_ref,
    arrived_ref,
    stay_ref,
    xsum_ref,
    part_ref,
    ysum_ref,
    got_ref,
    send_x,
    recv_x,
    send_y,
    recv_y,
    send_f,
    recv_f,
    send_m,
    recv_m,
):
    me_x, me_y = lax.axis_index("gx"), lax.axis_index("gy")
    places = meeting_places(nx, ny)
    greet(places)
    xsum_ref[me_x] = totals_ref[...]
    pl.semaphore_wait(pltpu.get_barrier_semaphore(), len(places))

    def copy(source, target, sends, recvs, n, dx, dy):
        made = pltpu.make_async_remote_copy(
            src_ref=source,
            dst_ref=target,
            send_sem=sends.at[n],
            recv_sem=recvs.at[n],
            device_id=(moved_by("gx", dx), moved_by("gy", dy)),
            device_id_type=MESH,
        )
        made.start()
        return made

    along_x = [
        copy(totals_ref, xsum_ref.at[me_x], send_x, recv_x, o - 1, o, 0) for o in range(1, nx)
    ]
    moving = [
        copy(packed_ref.at[k, pl.ds(cap, 16)], got_ref.at[k], send_m, recv_m, k, dx, dy)
        for k, (dx, dy) in enumerate(directions)
    ]
    feats = [
        copy(
            packed_ref.at[k, pl.ds(0, cap)],
            feat_ref.at[pl.ds(k * cap, cap)],
            send_f,
            recv_f,
            k,
            dx,
            dy,
        )
        for k, (dx, dy) in enumerate(directions)
    ]
    for made in along_x:
        made.wait()
    part = jnp.sum(xsum_ref[...], axis=0)
    part_ref[...] = part
    ysum_ref[me_y] = part
    along_y = [
        copy(part_ref, ysum_ref.at[me_y], send_y, recv_y, o - 1, 0, o) for o in range(1, ny)
    ]
    for made in along_y:
        made.wait()
    sums = jnp.sum(jnp.sum(ysum_ref[...], axis=0), axis=1, keepdims=True)
    drift = sums[:3] / sums[3:4]
    stay_ref[...] = jnp.where(dest_ref[...] == 0, vel1_ref[...] - drift, 0.0)
    for made in moving:
        made.wait()
    for k in range(len(directions)):
        values = got_ref[k].astype(jnp.float32)
        weight = values[3:4]
        slots = slice(k * cap, (k + 1) * cap)
        arrived_ref[:3, slots] = jnp.where(weight > 0, values[:3] - drift, 0.0)
        arrived_ref[3:4, slots] = weight
    for made in feats:
        made.wait()


def whole(shape):
    return pl.BlockSpec(shape, lambda g: (0,) * len(shape))


def shards(
    mesh_state,
    part_feat,
    cell_index,
    pairs,
    dest,
    mass,
    velocity,
    w_enc,
    w_mesh,
    w_pair,
    w_edge,
    w_node,
    w_accel,
):
    shape = mesh_state.shape
    parts, width = part_feat.shape
    cx, cy, cz, channels = shape
    cells = cx * cy * cz
    plane = cy * cz
    members, count, span = group_sizes(parts, cells)
    planes = span // plane
    per_group = pairs.shape[1] // count
    cap = parts // 32
    nx, ny = lax.axis_size("gx"), lax.axis_size("gy")
    bf16, f32 = (jnp.bfloat16, jnp.float32)
    params = pltpu.CompilerParams(vmem_limit_bytes=VMEM_LIMIT)

    by_rows = pl.BlockSpec((members, width), lambda g: (g, 0))
    by_cells = pl.BlockSpec((span, channels), lambda g: (g, 0))
    by_row = pl.BlockSpec((1, members), lambda g: (0, g))
    by_tile = pl.BlockSpec((1, members // LANES, LANES), lambda g: (g, 0, 0))

    cell_tile = cell_index.reshape(count, members // LANES, LANES)
    dest_row = dest.reshape(1, parts)
    dest_tile = dest.reshape(count, members // LANES, LANES)
    mass_row = mass.reshape(1, parts)

    groups = 2
    turns = count // groups
    early = lambda g: jnp.minimum(g, turns - 1)
    anywhere = pl.BlockSpec(memory_space=pl.ANY)
    mesh1, edge_sum, xlo, xhi, ylo, yhi = pl.pallas_call(
        functools.partial(front_kernel, turns, plane, cz, CHUNK),
        grid=(count,),
        out_shape=(
            jax.ShapeDtypeStruct((cells, channels), bf16),
            jax.ShapeDtypeStruct((parts, width), bf16),
            jax.ShapeDtypeStruct((plane, channels), bf16),
            jax.ShapeDtypeStruct((plane, channels), bf16),
            jax.ShapeDtypeStruct((cx * cz, channels), bf16),
            jax.ShapeDtypeStruct((cx * cz, channels), bf16),
        ),
        in_specs=[
            pl.BlockSpec((1, groups * members), lambda g: (0, early(g))),
            pl.BlockSpec((groups, members // LANES, LANES), lambda g: (early(g), 0, 0)),
            pl.BlockSpec((groups * members, width), lambda g: (early(g), 0)),
            pl.BlockSpec((groups * span, channels), lambda g: (early(g), 0)),
            by_rows,
            pl.BlockSpec((2, per_group), lambda g: (0, g)),
            whole(w_enc.shape),
            whole(w_pair.shape),
            whole(w_edge.shape),
        ],
        out_specs=(
            pl.BlockSpec((groups * span, channels), lambda g: (early(g), 0)),
            by_rows,
            anywhere,
            anywhere,
            anywhere,
            anywhere,
        ),
        scratch_shapes=[
            pltpu.VMEM((2, plane, channels), bf16),
            pltpu.VMEM((2, cx * cz, channels), bf16),
            pltpu.VMEM((2 * width, width), bf16),
            pltpu.SemaphoreType.DMA((4,)),
            pltpu.SemaphoreType.DMA((4,)),
        ],
        compiler_params=pltpu.CompilerParams(
            vmem_limit_bytes=VMEM_LIMIT, collective_id=0, has_side_effects=True
        ),
        name="front",
    )(
        cell_index.reshape(1, parts),
        cell_tile,
        part_feat,
        mesh_state.reshape(cells, channels),
        part_feat,
        pairs,
        w_enc,
        w_pair,
        w_edge,
    )

    one_plane = lambda f: pl.BlockSpec((plane, channels), f)
    by_layer = pl.BlockSpec((planes * cz, channels), lambda g: (g, 0))
    by_speed = pl.BlockSpec((3, members), lambda g: (0, g))
    mesh2, stay_feat, vel1, packed, totals = pl.pallas_call(
        functools.partial(node_kernel, plane, cz, cap),
        grid=(count,),
        out_shape=(
            jax.ShapeDtypeStruct((cells, channels), bf16),
            jax.ShapeDtypeStruct((parts, width), bf16),
            jax.ShapeDtypeStruct((3, parts), f32),
            jax.ShapeDtypeStruct((8, cap + 16, width), bf16),
            jax.ShapeDtypeStruct((4, LANES), f32),
        ),
        in_specs=[
            one_plane(lambda g: (jnp.maximum(g * planes - 1, 0), 0)),
            by_cells,
            one_plane(lambda g: (jnp.minimum(g * planes + planes, cx - 1), 0)),
            whole((plane, channels)),
            whole((plane, channels)),
            by_layer,
            by_layer,
            by_tile,
            by_tile,
            by_row,
            by_rows,
            by_rows,
            by_row,
            by_speed,
            whole(w_mesh.shape),
            whole(w_node.shape),
            whole(w_accel.shape),
        ],
        out_specs=(
            by_cells,
            by_rows,
            by_speed,
            whole((8, cap + 16, width)),
            whole((4, LANES)),
        ),
        scratch_shapes=[
            pltpu.VMEM((8 * cap, width + LANES), bf16),
            pltpu.VMEM((8, LANES), f32),
            pltpu.VMEM((2 * LANES, 2 * LANES), bf16),
            pltpu.VMEM((2 * width, 2 * width), bf16),
            pltpu.VMEM(w_node.shape, bf16),
            pltpu.VMEM((LANES, LANES), bf16),
        ],
        compiler_params=params,
        name="nodes",
    )(
        mesh1,
        mesh1,
        mesh1,
        xlo,
        xhi,
        ylo,
        yhi,
        cell_tile,
        dest_tile,
        dest_row,
        edge_sum,
        part_feat,
        mass_row,
        velocity,
        w_mesh,
        w_node,
        w_accel,
    )

    inside = pl.BlockSpec(memory_space=pltpu.VMEM)
    dma = lambda n: pltpu.SemaphoreType.DMA((n,))
    arrived_feat, arrived_vel, stay_vel = pl.pallas_call(
        functools.partial(tail_kernel, nx, ny, cap),
        out_shape=(
            jax.ShapeDtypeStruct((8 * cap, width), bf16),
            jax.ShapeDtypeStruct((4, 8 * cap), f32),
            jax.ShapeDtypeStruct((3, parts), f32),
        ),
        in_specs=[inside] * 4,
        out_specs=(anywhere, inside, inside),
        scratch_shapes=[
            pltpu.VMEM((nx, 4, LANES), f32),
            pltpu.VMEM((4, LANES), f32),
            pltpu.VMEM((ny, 4, LANES), f32),
            pltpu.VMEM((8, 16, LANES), bf16),
            dma(nx - 1),
            dma(nx - 1),
            dma(ny - 1),
            dma(ny - 1),
            dma(8),
            dma(8),
            dma(8),
            dma(8),
        ],
        compiler_params=pltpu.CompilerParams(
            vmem_limit_bytes=16 * 1024 * 1024, collective_id=1, has_side_effects=True
        ),
        name="tail",
    )(packed, totals, vel1, dest_row)
    return (mesh2.reshape(shape), stay_feat, stay_vel, arrived_feat, arrived_vel)


def solution(mesh):
    placed = (
        P("gx", "gy", None, None),
        P(("gx", "gy"), None),
        P(("gx", "gy")),
        P(None, ("gx", "gy")),
        P(("gx", "gy")),
        P(("gx", "gy")),
        P(None, ("gx", "gy")),
        P(),
        P(),
        P(),
        P(),
        P(),
        P(),
    )
    return jax.shard_map(
        shards,
        mesh=mesh,
        in_specs=placed,
        out_specs=(
            P("gx", "gy", None, None),
            P(("gx", "gy"), None),
            P(None, ("gx", "gy")),
            P(("gx", "gy"), None),
            P(None, ("gx", "gy")),
        ),
        check_vma=False,
    )
```

```python
import functools
import jax
import jax.numpy as jnp
from jax import lax
from jax.experimental import pallas as pl
from jax.experimental.pallas import tpu as pltpu
from jax.sharding import PartitionSpec as P

directions = ((-1, -1), (-1, 0), (-1, 1), (0, -1), (0, 1), (1, -1), (1, 0), (1, 1))
LANES = 128
VMEM_LIMIT = 28 * 1024 * 1024
CHUNK = 512
EDGE_GROUPS = 2
NODE_GROUPS = 2
FLIP = True
MESH = pl.DeviceIdType.MESH


def group_sizes(parts, cells):
    members = min(512, parts)
    count = parts // members
    return (members, count, cells // count)


def silu_of_twice(half):
    return half + half * jnp.tanh(half)


def wide(rows):
    return rows.astype(jnp.float32)


def f32dot(a, b):
    return jnp.dot(a, b, preferred_element_type=jnp.float32)


def nt_dot(a, b):
    return lax.dot_general(a, b, (((1,), (1,)), ((), ())), preferred_element_type=jnp.float32)


def down_hot(keys, rows):
    place = lax.broadcasted_iota(jnp.int32, (rows, keys.shape[1]), 0).astype(jnp.float32)
    place = place.astype(jnp.bfloat16)
    keys = keys.astype(jnp.float32).astype(jnp.bfloat16)
    one = jnp.ones((), jnp.bfloat16)
    return jnp.where(place == keys, one, jnp.zeros((), jnp.bfloat16))


def over_hot(keys, width):
    place = lax.broadcasted_iota(jnp.int32, (keys.shape[0], width), 1).astype(jnp.int16)
    keys = jnp.broadcast_to(keys, (keys.shape[0], LANES)).astype(jnp.int16)
    keys = jnp.concatenate([keys] * (width // LANES), axis=1)
    return jnp.where(place == keys, jnp.ones((), jnp.bfloat16), jnp.zeros((), jnp.bfloat16))


def moved_by(axis, distance):
    return lax.rem(lax.axis_index(axis) + distance + lax.axis_size(axis), lax.axis_size(axis))


def greet(places):
    barrier = pltpu.get_barrier_semaphore()
    for dx, dy in places:
        where = (moved_by("gx", dx), moved_by("gy", dy))
        pl.semaphore_signal(barrier, inc=1, device_id=where, device_id_type=MESH)


def front_kernel(
    turns,
    plane,
    depth,
    chunk,
    cell_ref,
    cell_tile_ref,
    enc_feat_ref,
    state_ref,
    feat_ref,
    pairs_ref,
    w_both_ref,
    mesh1_ref,
    edge_ref,
    xlo_ref,
    xhi_ref,
    ylo_ref,
    yhi_ref,
    xsend_ref,
    ysend_ref,
    half_pair_ref,
    send_sems,
    recv_sems,
):
    turn = pl.program_id(0)
    last = pl.num_programs(0) - 1
    width = feat_ref.shape[1]
    members = feat_ref.shape[0] // EDGE_GROUPS
    groups = cell_tile_ref.shape[0]
    span = state_ref.shape[0] // groups
    planes = state_ref.shape[0] // plane
    beside = ((1, 0), (-1, 0), (0, 1), (0, -1))
    half = members // 2

    def copies():
        sources = (xsend_ref.at[0], xsend_ref.at[1], ysend_ref.at[0], ysend_ref.at[1])
        targets = (xlo_ref, xhi_ref, ylo_ref, yhi_ref)
        return [
            pltpu.make_async_remote_copy(
                src_ref=sources[k],
                dst_ref=targets[k],
                send_sem=send_sems.at[k],
                recv_sem=recv_sems.at[k],
                device_id=(moved_by("gx", dx), moved_by("gy", dy)),
                device_id_type=MESH,
            )
            for k, (dx, dy) in enumerate(beside)
        ]

    @pl.when(turn == 0)
    def _():
        greet(beside)
        half_pair_ref[...] = (0.5 * w_both_ref[:, width:].astype(jnp.float32)).T.astype(jnp.bfloat16)

    @pl.when(turn < turns)
    def _():
        top = span // 2
        for g in range(groups):
            base = (turn * groups + g) * span
            mine = slice(g * members, (g + 1) * members)
            cols = (cell_tile_ref[g] - base).T
            grown = f32dot(enc_feat_ref[mine, :], w_both_ref[:, :width])
            low, high = [], []
            for j in range(members // LANES):
                rows = grown[j * LANES : (j + 1) * LANES]
                upper = cols[:, j : j + 1] >= top
                low.append(jnp.where(upper, 0.0, rows))
                high.append(jnp.where(upper, rows, 0.0))
            both = jnp.concatenate(
                [jnp.concatenate(low, axis=0), jnp.concatenate(high, axis=0)], axis=1
            ).astype(jnp.bfloat16)
            cells = cell_ref[:, mine] - base
            keys = jnp.where(cells >= top, cells - top, cells)
            for q in range(top // half):
                gain = f32dot(down_hot(keys - q * half, half), both)
                for part in range(2):
                    first = g * span + part * top + q * half
                    rows = slice(first, first + half)
                    mesh1_ref[rows, :] = (
                        state_ref[rows, :].astype(jnp.float32)
                        + gain[:, part * width : (part + 1) * width]
                    ).astype(jnp.bfloat16)
        for p in range(planes):
            first = p * plane
            rows = pl.ds(pl.multiple_of((turn * planes + p) * depth, depth), depth)
            ysend_ref[0, rows, :] = mesh1_ref[first + plane - depth : first + plane, :]
            ysend_ref[1, rows, :] = mesh1_ref[first : first + depth, :]

    @pl.when(turn == 0)
    def _():
        xsend_ref[1] = mesh1_ref[:plane, :]

    @pl.when(turn == turns - 1)
    def _():
        xsend_ref[0] = mesh1_ref[(planes - 1) * plane :, :]

    @pl.when(turn == turns - 1)
    def _():
        pl.semaphore_wait(pltpu.get_barrier_semaphore(), len(beside))
        for copy in copies():
            copy.start()

    totals = [jnp.zeros((half, 2 * width), jnp.float32)] * EDGE_GROUPS
    tables = []
    for g in range(EDGE_GROUPS):
        table = nt_dot(half_pair_ref[...], feat_ref[g * members : (g + 1) * members, :])
        table = table.astype(jnp.bfloat16)
        tables.append(jnp.concatenate([table[:width], table[width:]], axis=1))
    per_group = pairs_ref.shape[1] // EDGE_GROUPS
    for first in range(0, per_group, chunk):
        for g in range(EDGE_GROUPS):
            base = (turn * EDGE_GROUPS + g) * members
            start = g * per_group + first
            senders = pairs_ref[0:1, start : start + chunk] - base
            receivers = pairs_ref[1:2, start : start + chunk] - base
            upper = receivers >= half
            hots = [down_hot(senders, half), down_hot(senders - half, half)]
            hots += [down_hot(receivers, half), down_hot(receivers - half, half)]
            hot = hots[2] + hots[3]
            pre = f32dot(tables[g], jnp.concatenate(hots, axis=0))
            act = silu_of_twice(pre).astype(jnp.bfloat16)
            share = jnp.where(upper, 1.0, 0.0)
            acts = jnp.concatenate(
                [act * (1.0 - share).astype(jnp.bfloat16), act * share.astype(jnp.bfloat16)],
                axis=0,
            )
            if FLIP:
                totals[g] = totals[g] + nt_dot(acts, hot)
            else:
                totals[g] = totals[g] + nt_dot(hot, acts)
    for g in range(EDGE_GROUPS):
        total = totals[g].T if FLIP else totals[g]
        total = jnp.concatenate([total[:, :width], total[:, width:]], axis=0)
        edge_ref[g * members : (g + 1) * members, :] = total.astype(jnp.bfloat16)

    @pl.when(turn == last)
    def _():
        for copy in copies():
            copy.wait()


def node_kernel(
    plane,
    depth,
    cap,
    below_ref,
    centre_ref,
    above_ref,
    xlo_ref,
    xhi_ref,
    ylo_ref,
    yhi_ref,
    cell_ref,
    dest_ref,
    dest_row_ref,
    edge_ref,
    feat_ref,
    mass_ref,
    vel_ref,
    w_mesh_ref,
    w_edge_ref,
    w_node_ref,
    w_accel_ref,
    mesh_ref,
    stay_ref,
    vel1_ref,
    packed_ref,
    total_ref,
    slots_ref,
    carry_ref,
    near_w_ref,
    wide_w_ref,
    node_w_ref,
    before_ref,
    push_w_ref,
):
    step = pl.program_id(0)
    last = pl.num_programs(0) - 1
    width = centre_ref.shape[1]
    span = centre_ref.shape[0] // NODE_GROUPS
    members = feat_ref.shape[0] // NODE_GROUPS
    planes = centre_ref.shape[0] // plane
    block = 2 * LANES

    @pl.when(step == 0)
    def _():
        slots_ref[...] = jnp.zeros_like(slots_ref)
        carry_ref[...] = jnp.zeros_like(carry_ref)
        total_ref[...] = jnp.zeros_like(total_ref)
        row = lax.broadcasted_iota(jnp.int32, (block, block), 0)
        col = lax.broadcasted_iota(jnp.int32, (block, block), 1)
        gap = row - col
        up_down = (jnp.abs(gap) == 1) & (row // depth == col // depth)
        near_w_ref[...] = jnp.where(up_down | (jnp.abs(gap) == depth), 1.0, 0.0).astype(
            jnp.bfloat16
        )
        scaled = 0.5 * w_mesh_ref[...].astype(jnp.float32)
        none = jnp.zeros_like(scaled)
        wide_w_ref[...] = jnp.concatenate(
            [
                jnp.concatenate([scaled, none], axis=1),
                jnp.concatenate([none, scaled], axis=1),
            ],
            axis=0,
        ).astype(jnp.bfloat16)
        node_w_ref[...] = (0.5 * w_node_ref[...].astype(jnp.float32)).astype(jnp.bfloat16)
        push = jnp.concatenate(
            [wide(w_accel_ref[...]), jnp.zeros((LANES - 3, width), jnp.float32)], axis=0
        )
        push_w_ref[...] = push.T.astype(jnp.bfloat16)
        before_ref[...] = jnp.where(
            lax.broadcasted_iota(jnp.int32, (LANES, LANES), 0)
            < lax.broadcasted_iota(jnp.int32, (LANES, LANES), 1),
            1.0,
            0.0,
        ).astype(jnp.bfloat16)

    for p in range(planes):
        for pair in range(0, plane, 2 * block):
            firsts = [p * plane + pair, p * plane + pair + block]
            raw = [centre_ref[f : f + block, :] for f in firsts]
            around = f32dot(near_w_ref[...], jnp.concatenate(raw, axis=1))
            sides = []
            for n, f in enumerate(firsts):
                rows = slice(f, f + block)
                inner = slice(f - p * plane, f - p * plane + block)
                if p == 0:
                    below = jnp.where(step == 0, xlo_ref[inner, :], below_ref[inner, :])
                else:
                    below = centre_ref[f - plane : f - plane + block, :]
                if p == planes - 1:
                    above = jnp.where(step == last, xhi_ref[inner, :], above_ref[inner, :])
                else:
                    above = centre_ref[f + plane : f + plane + block, :]
                if inner.start == 0:
                    left = ylo_ref[p * depth : (p + 1) * depth, :]
                else:
                    left = centre_ref[f - depth : f, :]
                if inner.stop == plane:
                    right = yhi_ref[p * depth : (p + 1) * depth, :]
                else:
                    right = centre_ref[f + block : f + block + depth, :]
                total = around[:, n * width : (n + 1) * width] + (wide(below) + wide(above))
                sides.append(
                    jnp.concatenate(
                        [
                            total[:depth] + wide(left),
                            total[depth:-depth],
                            total[-depth:] + wide(right),
                        ],
                        axis=0,
                    ).astype(jnp.bfloat16)
                )
            gain = silu_of_twice(f32dot(jnp.concatenate(sides, axis=1), wide_w_ref[...]))
            for n, f in enumerate(firsts):
                mesh_ref[f : f + block, :] = (
                    wide(raw[n]) + gain[:, n * width : (n + 1) * width]
                ).astype(jnp.bfloat16)

    turns = members // LANES
    top = span // 2
    some = 2 * LANES
    items = [(g, start) for start in range(0, members, some) for g in range(NODE_GROUPS)]
    pairs, cell_cols, dest_cols = [], [], []
    for g in range(NODE_GROUPS):
        cells = g * span
        pairs.append(
            jnp.concatenate(
                [mesh_ref[cells : cells + top, :], mesh_ref[cells + top : cells + span, :]], axis=1
            )
        )
        cell_cols.append((cell_ref[g] - (step * NODE_GROUPS + g) * span).T)
        dest_cols.append(dest_ref[g].T)
    nears = {}
    for g, start in items:
        hots, uppers = [], []
        for j in range(start // LANES, (start + some) // LANES):
            col = cell_cols[g][:, j : j + 1]
            upper = col >= top
            uppers.append(upper)
            hots.append(over_hot(jnp.where(upper, col - top, col), top))
        found = f32dot(jnp.concatenate(hots, axis=0), pairs[g])
        nears[g, start] = jnp.concatenate(
            [
                jnp.where(
                    upper,
                    found[j * LANES : (j + 1) * LANES, width:],
                    found[j * LANES : (j + 1) * LANES, :width],
                )
                for j, upper in enumerate(uppers)
            ],
            axis=0,
        ).astype(jnp.bfloat16)
    parts = {}
    for g, start in items:
        rows = slice(g * members + start, g * members + start + some)
        edge_sum = f32dot(edge_ref[rows, :], w_edge_ref[...]).astype(jnp.bfloat16)
        update = f32dot(jnp.concatenate([edge_sum, nears[g, start]], axis=1), node_w_ref[...])
        parts[g, start] = (wide(feat_ref[rows, :]) + silu_of_twice(update)).astype(jnp.bfloat16)
    pushed = {item: f32dot(parts[item], push_w_ref[...]) for item in items}
    done = carry_ref[:, :1]
    all_values, all_places = [], []
    for g in range(NODE_GROUPS):
        mine = slice(g * members, (g + 1) * members)
        starts = range(0, members, some)
        h_new = jnp.concatenate([parts[g, start] for start in starts], axis=0)
        mass = mass_ref[:, mine]
        extra = jnp.concatenate(
            [vel_ref[:, mine], mass, jnp.zeros((LANES - 4, members), jnp.float32)], axis=0
        )
        extra = extra.T + jnp.concatenate([pushed[g, start] for start in starts], axis=0)
        all_values.append(jnp.concatenate([h_new, extra.astype(jnp.bfloat16)], axis=1))

        dest = dest_row_ref[:, mine]
        ways = lax.broadcasted_iota(jnp.int32, (8, members), 0) + 1
        chosen = jnp.where(ways == dest, 1.0, 0.0)
        stacked = jnp.concatenate(
            [chosen[:, j * LANES : (j + 1) * LANES] for j in range(turns)], axis=0
        )
        earlier = f32dot(stacked.astype(jnp.bfloat16), before_ref[...])
        counts = jnp.sum(stacked, axis=1, keepdims=True)
        places = []
        for j in range(turns):
            rows = slice(8 * j, 8 * (j + 1))
            places.append(jnp.where(stacked[rows] > 0, earlier[rows] + done, -1.0))
            done = done + counts[rows]
        all_places.append(jnp.concatenate(places, axis=1))
    carry_ref[...] = jnp.broadcast_to(done, carry_ref.shape)
    values = jnp.concatenate(all_values, axis=0)
    place = jnp.concatenate(all_places, axis=1)
    for k in range(8):
        rows = slice(k * cap, (k + 1) * cap)
        slots_ref[rows, :] += f32dot(down_hot(place[k : k + 1], cap), values).astype(jnp.bfloat16)
    for g in range(NODE_GROUPS):
        mine = slice(g * members, (g + 1) * members)
        mass = mass_ref[:, mine]
        vel1 = vel_ref[:, mine] + nt_dot(w_accel_ref[...], all_values[g][:, :width])
        vel1_ref[:, mine] = vel1
        sums = jnp.concatenate([mass * vel1, mass], axis=0)
        total_ref[...] += sum(sums[:, j * LANES : (j + 1) * LANES] for j in range(turns))
        for j in range(turns):
            rows = slice(j * LANES, (j + 1) * LANES)
            stay_ref[g * members + j * LANES : g * members + (j + 1) * LANES, :] = jnp.where(
                dest_cols[g][:, j : j + 1] == 0, wide(all_values[g][rows, :width]), 0.0
            ).astype(jnp.bfloat16)

    @pl.when(step == last)
    def _():
        moving = wide(slots_ref[:, width:]).T
        for k in range(8):
            rows = slice(k * cap, (k + 1) * cap)
            packed_ref[k, :cap, :] = slots_ref[rows, :width]
            packed_ref[k, cap:, :] = moving[:16, rows].astype(jnp.bfloat16)


def meeting_places(nx, ny):
    around = [(o, 0) for o in range(1, nx)] + [(0, o) for o in range(1, ny)]
    around += [(dx % nx, dy % ny) for dx, dy in directions]
    return [place for place in dict.fromkeys(around) if place != (0, 0)]


def tail_kernel(
    nx,
    ny,
    cap,
    packed_hbm,
    totals_hbm,
    vel1_hbm,
    dest_hbm,
    feat_ref,
    arrived_ref,
    stay_ref,
    packed_ref,
    totals_ref,
    vel1_ref,
    dest_ref,
    load_sems,
    xsum_ref,
    part_ref,
    ysum_ref,
    got_ref,
    send_x,
    recv_x,
    send_y,
    recv_y,
    send_f,
    recv_f,
    send_m,
    recv_m,
):
    me_x, me_y = lax.axis_index("gx"), lax.axis_index("gy")
    places = meeting_places(nx, ny)
    greet(places)
    loads = [
        pltpu.make_async_copy(source, target, load_sems.at[n])
        for n, (source, target) in enumerate(
            (
                (totals_hbm, totals_ref),
                (packed_hbm, packed_ref),
                (vel1_hbm, vel1_ref),
                (dest_hbm, dest_ref),
            )
        )
    ]
    for load in loads:
        load.start()
    loads[0].wait()
    xsum_ref[me_x] = totals_ref[...]
    pl.semaphore_wait(pltpu.get_barrier_semaphore(), len(places))

    def copy(source, target, sends, recvs, n, dx, dy):
        made = pltpu.make_async_remote_copy(
            src_ref=source,
            dst_ref=target,
            send_sem=sends.at[n],
            recv_sem=recvs.at[n],
            device_id=(moved_by("gx", dx), moved_by("gy", dy)),
            device_id_type=MESH,
        )
        made.start()
        return made

    along_x = [
        copy(totals_ref, xsum_ref.at[me_x], send_x, recv_x, o - 1, o, 0) for o in range(1, nx)
    ]
    loads[1].wait()
    moving = [
        copy(packed_ref.at[k, pl.ds(cap, 16)], got_ref.at[k], send_m, recv_m, k, dx, dy)
        for k, (dx, dy) in enumerate(directions)
    ]
    feats = [
        copy(
            packed_ref.at[k, pl.ds(0, cap)],
            feat_ref.at[pl.ds(k * cap, cap)],
            send_f,
            recv_f,
            k,
            dx,
            dy,
        )
        for k, (dx, dy) in enumerate(directions)
    ]
    for made in along_x:
        made.wait()
    part = jnp.sum(xsum_ref[...], axis=0)
    part_ref[...] = part
    ysum_ref[me_y] = part
    along_y = [
        copy(part_ref, ysum_ref.at[me_y], send_y, recv_y, o - 1, 0, o) for o in range(1, ny)
    ]
    for made in along_y:
        made.wait()
    sums = jnp.sum(jnp.sum(ysum_ref[...], axis=0), axis=1, keepdims=True)
    drift = sums[:3] / sums[3:4]
    loads[2].wait()
    loads[3].wait()
    stay_ref[...] = jnp.where(dest_ref[...] == 0, vel1_ref[...] - drift, 0.0)
    for made in moving:
        made.wait()
    for k in range(len(directions)):
        values = got_ref[k].astype(jnp.float32)
        weight = values[3:4]
        slots = slice(k * cap, (k + 1) * cap)
        arrived_ref[:3, slots] = jnp.where(weight > 0, values[:3] - drift, 0.0)
        arrived_ref[3:4, slots] = weight
    for made in feats:
        made.wait()


def whole(shape):
    return pl.BlockSpec(shape, lambda g: (0,) * len(shape))


def shards(
    mesh_state,
    part_feat,
    cell_index,
    pairs,
    dest,
    mass,
    velocity,
    w_enc,
    w_mesh,
    w_pair,
    w_edge,
    w_node,
    w_accel,
):
    shape = mesh_state.shape
    parts, width = part_feat.shape
    cx, cy, cz, channels = shape
    cells = cx * cy * cz
    plane = cy * cz
    members, count, span = group_sizes(parts, cells)
    planes = span // plane
    per_group = pairs.shape[1] // count
    cap = parts // 32
    nx, ny = lax.axis_size("gx"), lax.axis_size("gy")
    bf16, f32 = (jnp.bfloat16, jnp.float32)
    params = pltpu.CompilerParams(vmem_limit_bytes=VMEM_LIMIT)

    by_rows = pl.BlockSpec((members, width), lambda g: (g, 0))
    by_cells = pl.BlockSpec((span, channels), lambda g: (g, 0))
    by_row = pl.BlockSpec((1, members), lambda g: (0, g))
    by_tile = pl.BlockSpec((1, members // LANES, LANES), lambda g: (g, 0, 0))

    cell_tile = cell_index.reshape(count, members // LANES, LANES)
    dest_row = dest.reshape(1, parts)
    dest_tile = dest.reshape(count, members // LANES, LANES)
    mass_row = mass.reshape(1, parts)

    w_both = jnp.concatenate([w_enc, w_pair], axis=1)
    groups = 2 * EDGE_GROUPS
    turns = count // groups
    early = lambda g: jnp.minimum(g, turns - 1)
    anywhere = pl.BlockSpec(memory_space=pl.ANY)
    mesh1, edge_sum, xlo, xhi, ylo, yhi = pl.pallas_call(
        functools.partial(front_kernel, turns, plane, cz, CHUNK),
        grid=(count // EDGE_GROUPS,),
        out_shape=(
            jax.ShapeDtypeStruct((cells, channels), bf16),
            jax.ShapeDtypeStruct((parts, width), bf16),
            jax.ShapeDtypeStruct((plane, channels), bf16),
            jax.ShapeDtypeStruct((plane, channels), bf16),
            jax.ShapeDtypeStruct((cx * cz, channels), bf16),
            jax.ShapeDtypeStruct((cx * cz, channels), bf16),
        ),
        in_specs=[
            pl.BlockSpec((1, groups * members), lambda g: (0, early(g))),
            pl.BlockSpec((groups, members // LANES, LANES), lambda g: (early(g), 0, 0)),
            pl.BlockSpec((groups * members, width), lambda g: (early(g), 0)),
            pl.BlockSpec((groups * span, channels), lambda g: (early(g), 0)),
            pl.BlockSpec((EDGE_GROUPS * members, width), lambda g: (g, 0)),
            pl.BlockSpec((2, EDGE_GROUPS * per_group), lambda g: (0, g)),
            whole(w_both.shape),
        ],
        out_specs=(
            pl.BlockSpec((groups * span, channels), lambda g: (early(g), 0)),
            pl.BlockSpec((EDGE_GROUPS * members, width), lambda g: (g, 0)),
            anywhere,
            anywhere,
            anywhere,
            anywhere,
        ),
        scratch_shapes=[
            pltpu.VMEM((2, plane, channels), bf16),
            pltpu.VMEM((2, cx * cz, channels), bf16),
            pltpu.VMEM((2 * width, width), bf16),
            pltpu.SemaphoreType.DMA((4,)),
            pltpu.SemaphoreType.DMA((4,)),
        ],
        compiler_params=pltpu.CompilerParams(
            vmem_limit_bytes=VMEM_LIMIT, collective_id=0, has_side_effects=True
        ),
        name="front",
    )(
        cell_index.reshape(1, parts),
        cell_tile,
        part_feat,
        mesh_state.reshape(cells, channels),
        part_feat,
        pairs,
        w_both,
    )

    many = NODE_GROUPS
    by_rows = pl.BlockSpec((many * members, width), lambda g: (g, 0))
    by_cells = pl.BlockSpec((many * span, channels), lambda g: (g, 0))
    by_row = pl.BlockSpec((1, many * members), lambda g: (0, g))
    by_tile = pl.BlockSpec((many, members // LANES, LANES), lambda g: (g, 0, 0))
    planes = many * (span // plane)
    one_plane = lambda f: pl.BlockSpec((plane, channels), f)
    by_layer = pl.BlockSpec((planes * cz, channels), lambda g: (g, 0))
    by_speed = pl.BlockSpec((3, many * members), lambda g: (0, g))
    mesh2, stay_feat, vel1, packed, totals = pl.pallas_call(
        functools.partial(node_kernel, plane, cz, cap),
        grid=(count // many,),
        out_shape=(
            jax.ShapeDtypeStruct((cells, channels), bf16),
            jax.ShapeDtypeStruct((parts, width), bf16),
            jax.ShapeDtypeStruct((3, parts), f32),
            jax.ShapeDtypeStruct((8, cap + 16, width), bf16),
            jax.ShapeDtypeStruct((4, LANES), f32),
        ),
        in_specs=[
            one_plane(lambda g: (jnp.maximum(g * planes - 1, 0), 0)),
            by_cells,
            one_plane(lambda g: (jnp.minimum(g * planes + planes, cx - 1), 0)),
            whole((plane, channels)),
            whole((plane, channels)),
            by_layer,
            by_layer,
            by_tile,
            by_tile,
            by_row,
            by_rows,
            by_rows,
            by_row,
            by_speed,
            whole(w_mesh.shape),
            whole(w_edge.shape),
            whole(w_node.shape),
            whole(w_accel.shape),
        ],
        out_specs=(
            by_cells,
            by_rows,
            by_speed,
            whole((8, cap + 16, width)),
            whole((4, LANES)),
        ),
        scratch_shapes=[
            pltpu.VMEM((8 * cap, width + LANES), bf16),
            pltpu.VMEM((8, LANES), f32),
            pltpu.VMEM((2 * LANES, 2 * LANES), bf16),
            pltpu.VMEM((2 * width, 2 * width), bf16),
            pltpu.VMEM(w_node.shape, bf16),
            pltpu.VMEM((LANES, LANES), bf16),
            pltpu.VMEM((width, LANES), bf16),
        ],
        compiler_params=params,
        name="nodes",
    )(
        mesh1,
        mesh1,
        mesh1,
        xlo,
        xhi,
        ylo,
        yhi,
        cell_tile,
        dest_tile,
        dest_row,
        edge_sum,
        part_feat,
        mass_row,
        velocity,
        w_mesh,
        w_edge,
        w_node,
        w_accel,
    )

    inside = pl.BlockSpec(memory_space=pltpu.VMEM)
    dma = lambda n: pltpu.SemaphoreType.DMA((n,))
    arrived_feat, arrived_vel, stay_vel = pl.pallas_call(
        functools.partial(tail_kernel, nx, ny, cap),
        out_shape=(
            jax.ShapeDtypeStruct((8 * cap, width), bf16),
            jax.ShapeDtypeStruct((4, 8 * cap), f32),
            jax.ShapeDtypeStruct((3, parts), f32),
        ),
        in_specs=[pl.BlockSpec(memory_space=pltpu.HBM)] * 4,
        out_specs=(anywhere, inside, inside),
        scratch_shapes=[
            pltpu.VMEM(packed.shape, bf16),
            pltpu.VMEM(totals.shape, f32),
            pltpu.VMEM(vel1.shape, f32),
            pltpu.VMEM(dest_row.shape, jnp.int32),
            dma(4),
            pltpu.VMEM((nx, 4, LANES), f32),
            pltpu.VMEM((4, LANES), f32),
            pltpu.VMEM((ny, 4, LANES), f32),
            pltpu.VMEM((8, 16, LANES), bf16),
            dma(nx - 1),
            dma(nx - 1),
            dma(ny - 1),
            dma(ny - 1),
            dma(8),
            dma(8),
            dma(8),
            dma(8),
        ],
        compiler_params=pltpu.CompilerParams(
            vmem_limit_bytes=16 * 1024 * 1024, collective_id=1, has_side_effects=True
        ),
        name="tail",
    )(packed, totals, vel1, dest_row)
    return (mesh2.reshape(shape), stay_feat, stay_vel, arrived_feat, arrived_vel)


def solution(mesh):
    placed = (
        P("gx", "gy", None, None),
        P(("gx", "gy"), None),
        P(("gx", "gy")),
        P(None, ("gx", "gy")),
        P(("gx", "gy")),
        P(("gx", "gy")),
        P(None, ("gx", "gy")),
        P(),
        P(),
        P(),
        P(),
        P(),
        P(),
    )
    return jax.shard_map(
        shards,
        mesh=mesh,
        in_specs=placed,
        out_specs=(
            P("gx", "gy", None, None),
            P(("gx", "gy"), None),
            P(None, ("gx", "gy")),
            P(("gx", "gy"), None),
            P(None, ("gx", "gy")),
        ),
        check_vma=False,
    )
```

```python
import functools
import jax
import jax.numpy as jnp
from jax import lax
from jax.experimental import pallas as pl
from jax.experimental.pallas import tpu as pltpu
from jax.sharding import PartitionSpec as P

directions = ((-1, -1), (-1, 0), (-1, 1), (0, -1), (0, 1), (1, -1), (1, 0), (1, 1))
LANES = 128
VMEM_LIMIT = 28 * 1024 * 1024
CHUNK = 512
EDGE_GROUPS = 4
NODE_GROUPS = 4
FLIP = True
MESH = pl.DeviceIdType.MESH


def group_sizes(parts, cells):
    members = min(512, parts)
    count = parts // members
    return (members, count, cells // count)


def silu_of_twice(half):
    return half + half * jnp.tanh(half)


def wide(rows):
    return rows.astype(jnp.float32)


def f32dot(a, b):
    return jnp.dot(a, b, preferred_element_type=jnp.float32)


def nt_dot(a, b):
    return lax.dot_general(a, b, (((1,), (1,)), ((), ())), preferred_element_type=jnp.float32)


def down_hot(keys, rows):
    place = lax.broadcasted_iota(jnp.int32, (rows, keys.shape[1]), 0).astype(jnp.float32)
    place = place.astype(jnp.bfloat16)
    keys = keys.astype(jnp.float32).astype(jnp.bfloat16)
    one = jnp.ones((), jnp.bfloat16)
    return jnp.where(place == keys, one, jnp.zeros((), jnp.bfloat16))


def over_hot(keys, width):
    place = lax.broadcasted_iota(jnp.int32, (keys.shape[0], width), 1).astype(jnp.int16)
    keys = jnp.broadcast_to(keys, (keys.shape[0], LANES)).astype(jnp.int16)
    keys = jnp.concatenate([keys] * (width // LANES), axis=1)
    return jnp.where(place == keys, jnp.ones((), jnp.bfloat16), jnp.zeros((), jnp.bfloat16))


def moved_by(axis, distance):
    return lax.rem(lax.axis_index(axis) + distance + lax.axis_size(axis), lax.axis_size(axis))


def greet(places):
    barrier = pltpu.get_barrier_semaphore()
    for dx, dy in places:
        where = (moved_by("gx", dx), moved_by("gy", dy))
        pl.semaphore_signal(barrier, inc=1, device_id=where, device_id_type=MESH)


def front_kernel(
    turns,
    plane,
    depth,
    chunk,
    cell_ref,
    cell_tile_ref,
    enc_feat_ref,
    state_ref,
    feat_ref,
    pairs_ref,
    w_both_ref,
    mesh1_ref,
    edge_ref,
    xlo_ref,
    xhi_ref,
    ylo_ref,
    yhi_ref,
    xsend_ref,
    ysend_ref,
    half_pair_ref,
    send_sems,
    recv_sems,
):
    turn = pl.program_id(0)
    last = pl.num_programs(0) - 1
    width = feat_ref.shape[1]
    members = feat_ref.shape[0] // EDGE_GROUPS
    groups = cell_tile_ref.shape[0]
    span = state_ref.shape[0] // groups
    planes = state_ref.shape[0] // plane
    beside = ((1, 0), (-1, 0), (0, 1), (0, -1))
    half = members // 2

    def copies():
        sources = (xsend_ref.at[0], xsend_ref.at[1], ysend_ref.at[0], ysend_ref.at[1])
        targets = (xlo_ref, xhi_ref, ylo_ref, yhi_ref)
        return [
            pltpu.make_async_remote_copy(
                src_ref=sources[k],
                dst_ref=targets[k],
                send_sem=send_sems.at[k],
                recv_sem=recv_sems.at[k],
                device_id=(moved_by("gx", dx), moved_by("gy", dy)),
                device_id_type=MESH,
            )
            for k, (dx, dy) in enumerate(beside)
        ]

    @pl.when(turn == 0)
    def _():
        greet(beside)
        half_pair_ref[...] = (0.5 * w_both_ref[:, width:].astype(jnp.float32)).T.astype(jnp.bfloat16)

    @pl.when(turn < turns)
    def _():
        top = span // 2
        for g in range(groups):
            base = (turn * groups + g) * span
            mine = slice(g * members, (g + 1) * members)
            cols = (cell_tile_ref[g] - base).T
            grown = f32dot(enc_feat_ref[mine, :], w_both_ref[:, :width])
            low, high = [], []
            for j in range(members // LANES):
                rows = grown[j * LANES : (j + 1) * LANES]
                upper = cols[:, j : j + 1] >= top
                low.append(jnp.where(upper, 0.0, rows))
                high.append(jnp.where(upper, rows, 0.0))
            both = jnp.concatenate(
                [jnp.concatenate(low, axis=0), jnp.concatenate(high, axis=0)], axis=1
            ).astype(jnp.bfloat16)
            cells = cell_ref[:, mine] - base
            keys = jnp.where(cells >= top, cells - top, cells)
            for q in range(top // half):
                gain = f32dot(down_hot(keys - q * half, half), both)
                for part in range(2):
                    first = g * span + part * top + q * half
                    rows = slice(first, first + half)
                    mesh1_ref[rows, :] = (
                        state_ref[rows, :].astype(jnp.float32)
                        + gain[:, part * width : (part + 1) * width]
                    ).astype(jnp.bfloat16)
        for p in range(planes):
            first = p * plane
            rows = pl.ds(pl.multiple_of((turn * planes + p) * depth, depth), depth)
            ysend_ref[0, rows, :] = mesh1_ref[first + plane - depth : first + plane, :]
            ysend_ref[1, rows, :] = mesh1_ref[first : first + depth, :]

    @pl.when(turn == 0)
    def _():
        xsend_ref[1] = mesh1_ref[:plane, :]

    @pl.when(turn == turns - 1)
    def _():
        xsend_ref[0] = mesh1_ref[(planes - 1) * plane :, :]

    @pl.when(turn == turns - 1)
    def _():
        pl.semaphore_wait(pltpu.get_barrier_semaphore(), len(beside))
        for copy in copies():
            copy.start()

    totals = [jnp.zeros((half, 2 * width), jnp.float32)] * EDGE_GROUPS
    tables = []
    for g in range(EDGE_GROUPS):
        table = nt_dot(half_pair_ref[...], feat_ref[g * members : (g + 1) * members, :])
        table = table.astype(jnp.bfloat16)
        tables.append(jnp.concatenate([table[:width], table[width:]], axis=1))
    per_group = pairs_ref.shape[1] // EDGE_GROUPS
    for first in range(0, per_group, chunk):
        for g in range(EDGE_GROUPS):
            base = (turn * EDGE_GROUPS + g) * members
            start = g * per_group + first
            senders = pairs_ref[0:1, start : start + chunk] - base
            receivers = pairs_ref[1:2, start : start + chunk] - base
            upper = receivers >= half
            hots = [down_hot(senders, half), down_hot(senders - half, half)]
            hots += [down_hot(receivers, half), down_hot(receivers - half, half)]
            hot = hots[2] + hots[3]
            pre = f32dot(tables[g], jnp.concatenate(hots, axis=0))
            act = silu_of_twice(pre).astype(jnp.bfloat16)
            share = jnp.where(upper, 1.0, 0.0)
            acts = jnp.concatenate(
                [act * (1.0 - share).astype(jnp.bfloat16), act * share.astype(jnp.bfloat16)],
                axis=0,
            )
            if FLIP:
                totals[g] = totals[g] + nt_dot(acts, hot)
            else:
                totals[g] = totals[g] + nt_dot(hot, acts)
    for g in range(EDGE_GROUPS):
        total = totals[g].T if FLIP else totals[g]
        total = jnp.concatenate([total[:, :width], total[:, width:]], axis=0)
        edge_ref[g * members : (g + 1) * members, :] = total.astype(jnp.bfloat16)

    @pl.when(turn == last)
    def _():
        for copy in copies():
            copy.wait()


def node_kernel(
    plane,
    depth,
    cap,
    below_ref,
    centre_ref,
    above_ref,
    xlo_ref,
    xhi_ref,
    ylo_ref,
    yhi_ref,
    cell_ref,
    dest_ref,
    dest_row_ref,
    edge_ref,
    feat_ref,
    mass_ref,
    vel_ref,
    w_mesh_ref,
    w_edge_ref,
    w_node_ref,
    w_accel_ref,
    mesh_ref,
    stay_ref,
    vel1_ref,
    packed_ref,
    total_ref,
    slots_ref,
    carry_ref,
    near_w_ref,
    wide_w_ref,
    node_w_ref,
    before_ref,
    push_w_ref,
):
    step = pl.program_id(0)
    last = pl.num_programs(0) - 1
    width = centre_ref.shape[1]
    span = centre_ref.shape[0] // NODE_GROUPS
    members = feat_ref.shape[0] // NODE_GROUPS
    planes = centre_ref.shape[0] // plane
    block = 2 * LANES

    @pl.when(step == 0)
    def _():
        slots_ref[...] = jnp.zeros_like(slots_ref)
        carry_ref[...] = jnp.zeros_like(carry_ref)
        total_ref[...] = jnp.zeros_like(total_ref)
        row = lax.broadcasted_iota(jnp.int32, (block, block), 0)
        col = lax.broadcasted_iota(jnp.int32, (block, block), 1)
        gap = row - col
        up_down = (jnp.abs(gap) == 1) & (row // depth == col // depth)
        near_w_ref[...] = jnp.where(up_down | (jnp.abs(gap) == depth), 1.0, 0.0).astype(
            jnp.bfloat16
        )
        scaled = 0.5 * w_mesh_ref[...].astype(jnp.float32)
        none = jnp.zeros_like(scaled)
        wide_w_ref[...] = jnp.concatenate(
            [
                jnp.concatenate([scaled, none], axis=1),
                jnp.concatenate([none, scaled], axis=1),
            ],
            axis=0,
        ).astype(jnp.bfloat16)
        node_w_ref[...] = (0.5 * w_node_ref[...].astype(jnp.float32)).astype(jnp.bfloat16)
        push = jnp.concatenate(
            [wide(w_accel_ref[...]), jnp.zeros((LANES - 3, width), jnp.float32)], axis=0
        )
        push_w_ref[...] = push.T.astype(jnp.bfloat16)
        before_ref[...] = jnp.where(
            lax.broadcasted_iota(jnp.int32, (LANES, LANES), 0)
            < lax.broadcasted_iota(jnp.int32, (LANES, LANES), 1),
            1.0,
            0.0,
        ).astype(jnp.bfloat16)

    for p in range(planes):
        for pair in range(0, plane, 2 * block):
            firsts = [p * plane + pair, p * plane + pair + block]
            raw = [centre_ref[f : f + block, :] for f in firsts]
            around = f32dot(near_w_ref[...], jnp.concatenate(raw, axis=1))
            sides = []
            for n, f in enumerate(firsts):
                rows = slice(f, f + block)
                inner = slice(f - p * plane, f - p * plane + block)
                if p == 0:
                    below = jnp.where(step == 0, xlo_ref[inner, :], below_ref[inner, :])
                else:
                    below = centre_ref[f - plane : f - plane + block, :]
                if p == planes - 1:
                    above = jnp.where(step == last, xhi_ref[inner, :], above_ref[inner, :])
                else:
                    above = centre_ref[f + plane : f + plane + block, :]
                if inner.start == 0:
                    left = ylo_ref[p * depth : (p + 1) * depth, :]
                else:
                    left = centre_ref[f - depth : f, :]
                if inner.stop == plane:
                    right = yhi_ref[p * depth : (p + 1) * depth, :]
                else:
                    right = centre_ref[f + block : f + block + depth, :]
                total = around[:, n * width : (n + 1) * width] + (wide(below) + wide(above))
                sides.append(
                    jnp.concatenate(
                        [
                            total[:depth] + wide(left),
                            total[depth:-depth],
                            total[-depth:] + wide(right),
                        ],
                        axis=0,
                    ).astype(jnp.bfloat16)
                )
            gain = silu_of_twice(f32dot(jnp.concatenate(sides, axis=1), wide_w_ref[...]))
            for n, f in enumerate(firsts):
                mesh_ref[f : f + block, :] = (
                    wide(raw[n]) + gain[:, n * width : (n + 1) * width]
                ).astype(jnp.bfloat16)

    turns = members // LANES
    top = span // 2
    some = 2 * LANES
    items = [(g, start) for start in range(0, members, some) for g in range(NODE_GROUPS)]
    pairs, cell_cols, dest_cols = [], [], []
    for g in range(NODE_GROUPS):
        cells = g * span
        pairs.append(
            jnp.concatenate(
                [mesh_ref[cells : cells + top, :], mesh_ref[cells + top : cells + span, :]], axis=1
            )
        )
        cell_cols.append((cell_ref[g] - (step * NODE_GROUPS + g) * span).T)
        dest_cols.append(dest_ref[g].T)
    nears = {}
    for g, start in items:
        hots, uppers = [], []
        for j in range(start // LANES, (start + some) // LANES):
            col = cell_cols[g][:, j : j + 1]
            upper = col >= top
            uppers.append(upper)
            hots.append(over_hot(jnp.where(upper, col - top, col), top))
        found = f32dot(jnp.concatenate(hots, axis=0), pairs[g])
        nears[g, start] = jnp.concatenate(
            [
                jnp.where(
                    upper,
                    found[j * LANES : (j + 1) * LANES, width:],
                    found[j * LANES : (j + 1) * LANES, :width],
                )
                for j, upper in enumerate(uppers)
            ],
            axis=0,
        ).astype(jnp.bfloat16)
    parts = {}
    for g, start in items:
        rows = slice(g * members + start, g * members + start + some)
        edge_sum = f32dot(edge_ref[rows, :], w_edge_ref[...]).astype(jnp.bfloat16)
        update = f32dot(jnp.concatenate([edge_sum, nears[g, start]], axis=1), node_w_ref[...])
        parts[g, start] = (wide(feat_ref[rows, :]) + silu_of_twice(update)).astype(jnp.bfloat16)
    pushed = {item: f32dot(parts[item], push_w_ref[...]) for item in items}
    done = carry_ref[:, :1]
    all_values, all_places = [], []
    for g in range(NODE_GROUPS):
        mine = slice(g * members, (g + 1) * members)
        starts = range(0, members, some)
        h_new = jnp.concatenate([parts[g, start] for start in starts], axis=0)
        mass = mass_ref[:, mine]
        extra = jnp.concatenate(
            [vel_ref[:, mine], mass, jnp.zeros((LANES - 4, members), jnp.float32)], axis=0
        )
        extra = extra.T + jnp.concatenate([pushed[g, start] for start in starts], axis=0)
        all_values.append(jnp.concatenate([h_new, extra.astype(jnp.bfloat16)], axis=1))

        dest = dest_row_ref[:, mine]
        ways = lax.broadcasted_iota(jnp.int32, (8, members), 0) + 1
        chosen = jnp.where(ways == dest, 1.0, 0.0)
        stacked = jnp.concatenate(
            [chosen[:, j * LANES : (j + 1) * LANES] for j in range(turns)], axis=0
        )
        earlier = f32dot(stacked.astype(jnp.bfloat16), before_ref[...])
        counts = jnp.sum(stacked, axis=1, keepdims=True)
        places = []
        for j in range(turns):
            rows = slice(8 * j, 8 * (j + 1))
            places.append(jnp.where(stacked[rows] > 0, earlier[rows] + done, -1.0))
            done = done + counts[rows]
        all_places.append(jnp.concatenate(places, axis=1))
    carry_ref[...] = jnp.broadcast_to(done, carry_ref.shape)
    values = jnp.concatenate(all_values, axis=0)
    place = jnp.concatenate(all_places, axis=1)
    for k in range(8):
        rows = slice(k * cap, (k + 1) * cap)
        slots_ref[rows, :] += f32dot(down_hot(place[k : k + 1], cap), values).astype(jnp.bfloat16)
    for g in range(NODE_GROUPS):
        mine = slice(g * members, (g + 1) * members)
        mass = mass_ref[:, mine]
        vel1 = vel_ref[:, mine] + nt_dot(w_accel_ref[...], all_values[g][:, :width])
        vel1_ref[:, mine] = vel1
        sums = jnp.concatenate([mass * vel1, mass], axis=0)
        total_ref[...] += sum(sums[:, j * LANES : (j + 1) * LANES] for j in range(turns))
        for j in range(turns):
            rows = slice(j * LANES, (j + 1) * LANES)
            stay_ref[g * members + j * LANES : g * members + (j + 1) * LANES, :] = jnp.where(
                dest_cols[g][:, j : j + 1] == 0, wide(all_values[g][rows, :width]), 0.0
            ).astype(jnp.bfloat16)

    @pl.when(step == last)
    def _():
        moving = wide(slots_ref[:, width:]).T
        for k in range(8):
            rows = slice(k * cap, (k + 1) * cap)
            packed_ref[k, :cap, :] = slots_ref[rows, :width]
            packed_ref[k, cap:, :] = moving[:16, rows].astype(jnp.bfloat16)


def meeting_places(nx, ny):
    around = [(o, 0) for o in range(1, nx)] + [(0, o) for o in range(1, ny)]
    around += [(dx % nx, dy % ny) for dx, dy in directions]
    return [place for place in dict.fromkeys(around) if place != (0, 0)]


def tail_kernel(
    nx,
    ny,
    cap,
    packed_hbm,
    totals_hbm,
    vel1_hbm,
    dest_hbm,
    feat_ref,
    arrived_ref,
    stay_ref,
    packed_ref,
    totals_ref,
    vel1_ref,
    dest_ref,
    load_sems,
    xsum_ref,
    part_ref,
    ysum_ref,
    got_ref,
    send_x,
    recv_x,
    send_y,
    recv_y,
    send_f,
    recv_f,
    send_m,
    recv_m,
):
    me_x, me_y = lax.axis_index("gx"), lax.axis_index("gy")
    places = meeting_places(nx, ny)
    greet(places)
    loads = [
        pltpu.make_async_copy(source, target, load_sems.at[n])
        for n, (source, target) in enumerate(
            (
                (totals_hbm, totals_ref),
                (packed_hbm, packed_ref),
                (vel1_hbm, vel1_ref),
                (dest_hbm, dest_ref),
            )
        )
    ]
    for load in loads:
        load.start()
    loads[0].wait()
    xsum_ref[me_x] = totals_ref[...]
    pl.semaphore_wait(pltpu.get_barrier_semaphore(), len(places))

    def copy(source, target, sends, recvs, n, dx, dy):
        made = pltpu.make_async_remote_copy(
            src_ref=source,
            dst_ref=target,
            send_sem=sends.at[n],
            recv_sem=recvs.at[n],
            device_id=(moved_by("gx", dx), moved_by("gy", dy)),
            device_id_type=MESH,
        )
        made.start()
        return made

    along_x = [
        copy(totals_ref, xsum_ref.at[me_x], send_x, recv_x, o - 1, o, 0) for o in range(1, nx)
    ]
    loads[1].wait()
    moving = [
        copy(packed_ref.at[k, pl.ds(cap, 16)], got_ref.at[k], send_m, recv_m, k, dx, dy)
        for k, (dx, dy) in enumerate(directions)
    ]
    feats = [
        copy(
            packed_ref.at[k, pl.ds(0, cap)],
            feat_ref.at[pl.ds(k * cap, cap)],
            send_f,
            recv_f,
            k,
            dx,
            dy,
        )
        for k, (dx, dy) in enumerate(directions)
    ]
    for made in along_x:
        made.wait()
    part = jnp.sum(xsum_ref[...], axis=0)
    part_ref[...] = part
    ysum_ref[me_y] = part
    along_y = [
        copy(part_ref, ysum_ref.at[me_y], send_y, recv_y, o - 1, 0, o) for o in range(1, ny)
    ]
    for made in along_y:
        made.wait()
    sums = jnp.sum(jnp.sum(ysum_ref[...], axis=0), axis=1, keepdims=True)
    drift = sums[:3] / sums[3:4]
    loads[2].wait()
    loads[3].wait()
    stay_ref[...] = jnp.where(dest_ref[...] == 0, vel1_ref[...] - drift, 0.0)
    for made in moving:
        made.wait()
    for k in range(len(directions)):
        values = got_ref[k].astype(jnp.float32)
        weight = values[3:4]
        slots = slice(k * cap, (k + 1) * cap)
        arrived_ref[:3, slots] = jnp.where(weight > 0, values[:3] - drift, 0.0)
        arrived_ref[3:4, slots] = weight
    for made in feats:
        made.wait()


def whole(shape):
    return pl.BlockSpec(shape, lambda g: (0,) * len(shape))


def shards(
    mesh_state,
    part_feat,
    cell_index,
    pairs,
    dest,
    mass,
    velocity,
    w_enc,
    w_mesh,
    w_pair,
    w_edge,
    w_node,
    w_accel,
):
    shape = mesh_state.shape
    parts, width = part_feat.shape
    cx, cy, cz, channels = shape
    cells = cx * cy * cz
    plane = cy * cz
    members, count, span = group_sizes(parts, cells)
    planes = span // plane
    per_group = pairs.shape[1] // count
    cap = parts // 32
    nx, ny = lax.axis_size("gx"), lax.axis_size("gy")
    bf16, f32 = (jnp.bfloat16, jnp.float32)
    params = pltpu.CompilerParams(vmem_limit_bytes=VMEM_LIMIT)

    by_rows = pl.BlockSpec((members, width), lambda g: (g, 0))
    by_cells = pl.BlockSpec((span, channels), lambda g: (g, 0))
    by_row = pl.BlockSpec((1, members), lambda g: (0, g))
    by_tile = pl.BlockSpec((1, members // LANES, LANES), lambda g: (g, 0, 0))

    cell_tile = cell_index.reshape(count, members // LANES, LANES)
    dest_row = dest.reshape(1, parts)
    dest_tile = dest.reshape(count, members // LANES, LANES)
    mass_row = mass.reshape(1, parts)

    w_both = jnp.concatenate([w_enc, w_pair], axis=1)
    groups = 2 * EDGE_GROUPS
    turns = count // groups
    early = lambda g: jnp.minimum(g, turns - 1)
    anywhere = pl.BlockSpec(memory_space=pl.ANY)
    mesh1, edge_sum, xlo, xhi, ylo, yhi = pl.pallas_call(
        functools.partial(front_kernel, turns, plane, cz, CHUNK),
        grid=(count // EDGE_GROUPS,),
        out_shape=(
            jax.ShapeDtypeStruct((cells, channels), bf16),
            jax.ShapeDtypeStruct((parts, width), bf16),
            jax.ShapeDtypeStruct((plane, channels), bf16),
            jax.ShapeDtypeStruct((plane, channels), bf16),
            jax.ShapeDtypeStruct((cx * cz, channels), bf16),
            jax.ShapeDtypeStruct((cx * cz, channels), bf16),
        ),
        in_specs=[
            pl.BlockSpec((1, groups * members), lambda g: (0, early(g))),
            pl.BlockSpec((groups, members // LANES, LANES), lambda g: (early(g), 0, 0)),
            pl.BlockSpec((groups * members, width), lambda g: (early(g), 0)),
            pl.BlockSpec((groups * span, channels), lambda g: (early(g), 0)),
            pl.BlockSpec((EDGE_GROUPS * members, width), lambda g: (g, 0)),
            pl.BlockSpec((2, EDGE_GROUPS * per_group), lambda g: (0, g)),
            whole(w_both.shape),
        ],
        out_specs=(
            pl.BlockSpec((groups * span, channels), lambda g: (early(g), 0)),
            pl.BlockSpec((EDGE_GROUPS * members, width), lambda g: (g, 0)),
            anywhere,
            anywhere,
            anywhere,
            anywhere,
        ),
        scratch_shapes=[
            pltpu.VMEM((2, plane, channels), bf16),
            pltpu.VMEM((2, cx * cz, channels), bf16),
            pltpu.VMEM((2 * width, width), bf16),
            pltpu.SemaphoreType.DMA((4,)),
            pltpu.SemaphoreType.DMA((4,)),
        ],
        compiler_params=pltpu.CompilerParams(
            vmem_limit_bytes=VMEM_LIMIT, collective_id=0, has_side_effects=True
        ),
        name="front",
    )(
        cell_index.reshape(1, parts),
        cell_tile,
        part_feat,
        mesh_state.reshape(cells, channels),
        part_feat,
        pairs,
        w_both,
    )

    many = NODE_GROUPS
    by_rows = pl.BlockSpec((many * members, width), lambda g: (g, 0))
    by_cells = pl.BlockSpec((many * span, channels), lambda g: (g, 0))
    by_row = pl.BlockSpec((1, many * members), lambda g: (0, g))
    by_tile = pl.BlockSpec((many, members // LANES, LANES), lambda g: (g, 0, 0))
    planes = many * (span // plane)
    one_plane = lambda f: pl.BlockSpec((plane, channels), f)
    by_layer = pl.BlockSpec((planes * cz, channels), lambda g: (g, 0))
    by_speed = pl.BlockSpec((3, many * members), lambda g: (0, g))
    mesh2, stay_feat, vel1, packed, totals = pl.pallas_call(
        functools.partial(node_kernel, plane, cz, cap),
        grid=(count // many,),
        out_shape=(
            jax.ShapeDtypeStruct((cells, channels), bf16),
            jax.ShapeDtypeStruct((parts, width), bf16),
            jax.ShapeDtypeStruct((3, parts), f32),
            jax.ShapeDtypeStruct((8, cap + 16, width), bf16),
            jax.ShapeDtypeStruct((4, LANES), f32),
        ),
        in_specs=[
            one_plane(lambda g: (jnp.maximum(g * planes - 1, 0), 0)),
            by_cells,
            one_plane(lambda g: (jnp.minimum(g * planes + planes, cx - 1), 0)),
            whole((plane, channels)),
            whole((plane, channels)),
            by_layer,
            by_layer,
            by_tile,
            by_tile,
            by_row,
            by_rows,
            by_rows,
            by_row,
            by_speed,
            whole(w_mesh.shape),
            whole(w_edge.shape),
            whole(w_node.shape),
            whole(w_accel.shape),
        ],
        out_specs=(
            by_cells,
            by_rows,
            by_speed,
            whole((8, cap + 16, width)),
            whole((4, LANES)),
        ),
        scratch_shapes=[
            pltpu.VMEM((8 * cap, width + LANES), bf16),
            pltpu.VMEM((8, LANES), f32),
            pltpu.VMEM((2 * LANES, 2 * LANES), bf16),
            pltpu.VMEM((2 * width, 2 * width), bf16),
            pltpu.VMEM(w_node.shape, bf16),
            pltpu.VMEM((LANES, LANES), bf16),
            pltpu.VMEM((width, LANES), bf16),
        ],
        compiler_params=params,
        name="nodes",
    )(
        mesh1,
        mesh1,
        mesh1,
        xlo,
        xhi,
        ylo,
        yhi,
        cell_tile,
        dest_tile,
        dest_row,
        edge_sum,
        part_feat,
        mass_row,
        velocity,
        w_mesh,
        w_edge,
        w_node,
        w_accel,
    )

    inside = pl.BlockSpec(memory_space=pltpu.VMEM)
    dma = lambda n: pltpu.SemaphoreType.DMA((n,))
    arrived_feat, arrived_vel, stay_vel = pl.pallas_call(
        functools.partial(tail_kernel, nx, ny, cap),
        out_shape=(
            jax.ShapeDtypeStruct((8 * cap, width), bf16),
            jax.ShapeDtypeStruct((4, 8 * cap), f32),
            jax.ShapeDtypeStruct((3, parts), f32),
        ),
        in_specs=[pl.BlockSpec(memory_space=pltpu.HBM)] * 4,
        out_specs=(anywhere, inside, inside),
        scratch_shapes=[
            pltpu.VMEM(packed.shape, bf16),
            pltpu.VMEM(totals.shape, f32),
            pltpu.VMEM(vel1.shape, f32),
            pltpu.VMEM(dest_row.shape, jnp.int32),
            dma(4),
            pltpu.VMEM((nx, 4, LANES), f32),
            pltpu.VMEM((4, LANES), f32),
            pltpu.VMEM((ny, 4, LANES), f32),
            pltpu.VMEM((8, 16, LANES), bf16),
            dma(nx - 1),
            dma(nx - 1),
            dma(ny - 1),
            dma(ny - 1),
            dma(8),
            dma(8),
            dma(8),
            dma(8),
        ],
        compiler_params=pltpu.CompilerParams(
            vmem_limit_bytes=16 * 1024 * 1024, collective_id=1, has_side_effects=True
        ),
        name="tail",
    )(packed, totals, vel1, dest_row)
    return (mesh2.reshape(shape), stay_feat, stay_vel, arrived_feat, arrived_vel)


def solution(mesh):
    placed = (
        P("gx", "gy", None, None),
        P(("gx", "gy"), None),
        P(("gx", "gy")),
        P(None, ("gx", "gy")),
        P(("gx", "gy")),
        P(("gx", "gy")),
        P(None, ("gx", "gy")),
        P(),
        P(),
        P(),
        P(),
        P(),
        P(),
    )
    return jax.shard_map(
        shards,
        mesh=mesh,
        in_specs=placed,
        out_specs=(
            P("gx", "gy", None, None),
            P(("gx", "gy"), None),
            P(None, ("gx", "gy")),
            P(("gx", "gy"), None),
            P(None, ("gx", "gy")),
        ),
        check_vma=False,
    )
```
